32 devices in a mesh: row: 4 (over y, core), col: 8 (over z, x).
Axes of the slice: x: 2, y: 2, z: 4, core: 2. Of those that a mesh axis runs over, the one named last changes fastest.
Arguments:
- volume: float32 [8, 1024, 1024], P(None, 'row', 'col'), may hold values from -6 to 6
- ray_weights: float32 [16, 1024], P(None, 'row'), may hold values from 0.5 to 2
- shear_weights: bfloat16 [16, 128, 128], replicated, may hold values from -0.5 to 0.5
- shear_offsets: int32 [16], replicated, may hold values from 0 to 7
- measured: float32 [16, 8, 1024], P('row', None, 'col'), may hold values from -6 to 6
Outputs:
- residual: float32 [16, 8, 1024], P('row', None, 'col')
- gradient: float32 [8, 1024, 1024], P(None, 'row', 'col')
The draws below stay inside these ranges and needn't reach their ends.
All inputs are finite; a program needn't handle non-finite values.
Results may differ from the reference program's by a relative error of at most 0.0003.
Values sent between devices are 32-bit elements; how exact they have to be, the bound alone decides.
A program may use at most 64 MiB of HBM per device.

```python
import math
import jax
import jax.numpy as jnp
from jax import lax

CX = 256
CY = 128
SL = 8
NX = 1024
NY = 1024
ANGLES = 16
N_ROW = 4
N_COL = 8


def plant(values, key, smallest, high):
    extent = values.shape
    index_at = [jax.random.randint(jax.random.fold_in(key, axis), (), 0, extent[axis]) for axis in range(len(extent))]
    values = values.at[tuple(index_at)].set(smallest)
    longest = extent.index(max(extent))
    index_at[longest] = (index_at[longest] + 1) % extent[longest]
    return values.at[tuple(index_at)].set(high)


def steps_of(rng, dims, shards, smallest, high):
    factor_of, own = 1.0, jax.random.fold_in(rng, 6)
    for axis_at, parts in shards:
        heights = jnp.exp(jax.random.uniform(jax.random.fold_in(own, axis_at), (parts,), jnp.float32, smallest / len(shards), high / len(shards)))
        factor_of = factor_of * jnp.repeat(heights, dims[axis_at] // parts).reshape([-1 if axis == axis_at else 1 for axis in range(len(dims))])
    return factor_of


def noise(stream_key, dims, scale, bound, pieces=(), kind=jnp.bfloat16):
    array = scale * jax.random.normal(stream_key, dims, jnp.float32)
    if pieces:
        array = array * steps_of(stream_key, dims, pieces, -0.22, 0.18)
    return jnp.clip(array, -bound, bound).astype(kind)


def setup_inputs(seed: int = 0) -> dict:
    streams_of = jax.random.split(jax.random.key(seed), 6)
    volume = noise(streams_of[0], (SL, NX, NY), 1.0, 6.0, ((1, 4), (2, 8)), jnp.float32)
    ray_weights = jnp.clip(jnp.exp(math.log(2.0) - 1.3862944 * jax.random.uniform(streams_of[1], (ANGLES, NX), jnp.float32) ** steps_of(streams_of[1], (ANGLES, NX), ((1, 4),), -0.2, 0.2)), 0.5, 2.0)
    shear_weights = noise(streams_of[2], (ANGLES, CY, CY), CY ** -0.5, 0.5)
    shear_offsets = plant(jax.random.randint(streams_of[3], (ANGLES,), 0, N_COL), jax.random.fold_in(streams_of[3], 1), 0, N_COL - 1).astype(jnp.int32)
    measured = noise(streams_of[4], (ANGLES, SL, NY), 1.0, 6.0, ((0, 4), (2, 8)), jnp.float32)
    return dict(volume=volume, ray_weights=ray_weights, shear_weights=shear_weights, shear_offsets=shear_offsets, measured=measured)


def reference(volume, ray_weights, shear_weights, shear_offsets, measured):
    highest = lax.Precision.HIGHEST
    factor = 1.0 / math.sqrt(NX)
    blocks = volume.reshape(SL, N_ROW, CX, NY)
    weights_rows = ray_weights.reshape(ANGLES, N_ROW, CX)
    tilesum = jnp.einsum('arx,srxn->arsn', weights_rows, blocks, precision=highest) * factor
    shear = shear_weights.astype(jnp.float32)
    tiles = tilesum.reshape(ANGLES, N_ROW, SL, N_COL, CY)
    projected = jnp.einsum('arscy,ayz->arscz', tiles, shear, precision=highest)
    row_positions = jnp.arange(N_ROW, dtype=jnp.int32)
    col_positions = jnp.arange(N_COL, dtype=jnp.int32)
    moved = shear_offsets.astype(jnp.int32)[:, None, None] * row_positions[None, :, None]
    source = (col_positions[None, None, :] - moved) % N_COL
    full_shape = (ANGLES, N_ROW, SL, N_COL, CY)
    source_index = jnp.broadcast_to(source[:, :, None, :, None], full_shape).astype(jnp.int32)
    landed = jnp.take_along_axis(projected, source_index, axis=3)
    projection = lax.optimization_barrier(jnp.sum(landed, axis=1)).reshape(ANGLES, SL, NY)
    residual = projection - measured
    target = (col_positions[None, None, :] + moved) % N_COL
    target_index = jnp.broadcast_to(target[:, :, None, :, None], full_shape).astype(jnp.int32)
    resid_tiles = jnp.broadcast_to(residual.reshape(ANGLES, 1, SL, N_COL, CY), full_shape)
    pulled = jnp.take_along_axis(resid_tiles, target_index, axis=3)
    spread = jnp.einsum('arscz,ayz->arscy', pulled, shear, precision=highest)
    spread = spread.reshape(ANGLES, N_ROW, SL, NY)
    gradient = jnp.einsum('arx,arsn->srxn', weights_rows, spread, precision=highest) * factor
    return (residual, gradient.reshape(SL, NX, NY))
```

```python
import functools
import math

import jax
import jax.numpy as jnp
from jax import lax
from jax.experimental import pallas as pl
from jax.experimental.pallas import tpu as pltpu
from jax.sharding import PartitionSpec as P

MESH = pl.DeviceIdType.MESH
UNROLL_UP_TO = 64
KERNEL_VMEM = 24 * 1024 * 1024


def split(value):
    high = value.astype(jnp.bfloat16)
    return high, (value - high.astype(jnp.float32)).astype(jnp.bfloat16)


def each(count, body):
    if count <= UNROLL_UP_TO:
        for step in range(count):
            body(step)
    else:
        lax.fori_loop(0, count, lambda step, _: (body(step), 0)[1], 0)


def flip(index, step, size):
    if size & (size - 1):
        return lax.rem(index + step, size)
    bit = 1
    while bit < size:
        if step & bit:
            index = index + bit - 2 * bit * lax.rem(index // bit, 2)
        bit *= 2
    return index


def far_first(size):
    return sorted(range(1, size), key=lambda step: (-step.bit_count(), -step)) + [0]


def bytes_of(ref, blocks, sem):
    part = ref.at[pl.ds(0, blocks)]
    return pltpu.make_async_copy(part, part, sem)


class Homes:
    def __init__(self, rows, cols, angles):
        owned = angles // rows
        self.group = 2 if rows % 2 == 0 and owned % 2 == 0 else 1
        self.per = 2 if owned % 2 == 0 else 1
        self.beside = self.group * owned // self.per
        self.count = angles // self.per
        self.owned = owned
        self.base = (cols - self.beside) // 2

    def place(self, home):
        return home // self.beside * self.group + self.group - 1, self.base + lax.rem(home, self.beside)

    def owner(self, home):
        return home * self.per // self.owned


def exchange(
    rows, cols, factor, homes,
    volume_ref, weights_ref, shear_ref, offsets_ref, measured_ref,
    columns_ref, spread_ref, residual_ref,
    slab, weights_in, shear, offsets, measured, tiles, landed, measure_in, resid, spreads, pulls, pulled, resid_in,
    slab_sem, local_sem, out_sem, in_sem, back_out_sem, back_in_sem, m_out_sem, m_in_sem, r_out_sem, r_in_sem,
):
    slices = volume_ref.shape[0]
    angles = weights_ref.shape[0]
    owned = measured_ref.shape[0]
    width = volume_ref.shape[2]
    per, base, beside = homes.per, homes.base, homes.beside
    own_homes = owned // per
    count = rows * cols
    row, col = lax.axis_index("row"), lax.axis_index("col")
    me = row * cols + col
    at_home = jnp.logical_and(
        lax.rem(row, homes.group) == homes.group - 1, jnp.logical_and(col >= base, col < base + beside))
    away = jnp.logical_not(at_home)
    mine = row // homes.group * beside + lax.clamp(0, col - base, beside - 1)
    owner = homes.owner(mine)
    owner_here = jnp.logical_and(at_home, owner == row)
    owner_there = jnp.logical_and(at_home, owner != row)

    def device(index):
        return index // cols, lax.rem(index, cols)

    def others(body):
        if count <= UNROLL_UP_TO:
            for index in sorted(range(count), key=lambda index: (index % cols, index // cols)):
                pl.when(me != index)(functools.partial(body, index, (index // cols, index % cols)))
        else:
            def step(offset, carry):
                other = lax.rem(me + offset, count)
                body(other, device(other))
                return carry
            lax.fori_loop(1, count, step, 0)

    barrier = pltpu.get_barrier_semaphore()

    weights_copy = pltpu.make_async_copy(weights_ref, weights_in, local_sem.at[0])
    weights_copy.start()
    volume_copies = []
    for s in range(slices):
        copy = pltpu.make_async_copy(volume_ref.at[s], slab.at[s], slab_sem.at[s])
        copy.start()
        volume_copies.append(copy)

    @pl.when(at_home)
    def _():
        others(lambda index, place: pl.semaphore_signal(barrier, inc=1, device_id=place, device_id_type=MESH))

    measured_copy = pltpu.make_async_copy(measured_ref, measured, local_sem.at[2])
    measured_copy.start()
    shear_copy = pltpu.make_async_copy(shear_ref.at[pl.ds(mine * per, per)], shear, local_sem.at[1])
    shear_copy.start()
    offsets_copy = pltpu.make_async_copy(offsets_ref, offsets, local_sem.at[3])
    offsets_copy.start()

    weights_copy.wait()
    weights = weights_in[...] * factor
    w_high, w_low = split(weights)
    w_both = jnp.concatenate([w_high, w_low], axis=0)
    for s in range(slices):
        volume_copies[s].wait()
        v_high, v_low = split(slab[s])
        first = jnp.dot(w_both, v_high, preferred_element_type=jnp.float32)
        second = jnp.dot(w_high, v_low, preferred_element_type=jnp.float32)
        tiles[pl.ds(s, angles, stride=slices), :] = first[:angles] + first[angles:] + second
    measured_copy.wait()
    shear_copy.wait()
    offsets_copy.wait()

    @pl.when(at_home)
    def _():
        pl.semaphore_wait(barrier, homes.count - 1)

    @pl.when(away)
    def _():
        pl.semaphore_wait(barrier, homes.count)

    def send(source, target, send_sem, recv_sem, place):
        pltpu.make_async_remote_copy(
            src_ref=source, dst_ref=target, send_sem=send_sem, recv_sem=recv_sem,
            device_id=place, device_id_type=MESH).start()

    block = per * slices

    def send_tile(step):
        home = flip(mine, step, homes.count)
        send(tiles.at[pl.ds(home * block, block)], landed.at[me], out_sem, in_sem, homes.place(home))

    for step in far_first(homes.count)[:-1]:
        send_tile(step)
    pl.when(away)(functools.partial(send_tile, 0))

    for k in range(own_homes):
        home = row * own_homes + k
        place = homes.place(home)
        here = jnp.logical_and(place[0] == row, place[1] == col)

        @pl.when(jnp.logical_not(here))
        def _():
            send(measured.at[pl.ds(k * per, per)], measure_in.at[col], m_out_sem, m_in_sem, place)

        @pl.when(here)
        def _():
            measure_in[col] = measured[k * per:(k + 1) * per]

    columns_ref[...] = jnp.concatenate(
        [weights, weights - w_high.astype(jnp.float32), weights], axis=0).T.astype(jnp.bfloat16)

    @pl.when(at_home)
    def _():
        landed[me] = tiles[pl.ds(pl.multiple_of(mine * block, block), block), :]

    @pl.when(owner_here)
    def _():
        bytes_of(measure_in, cols - 1, m_in_sem).wait()

    @pl.when(owner_there)
    def _():
        bytes_of(measure_in, cols, m_in_sem).wait()

    @pl.when(at_home)
    def _():
        bytes_of(landed, count - 1, in_sem).wait()
        for slot in range(per):
            part = slice(slot * slices, (slot + 1) * slices)
            offset = offsets[mine * per + slot]
            totals = []
            for c in range(cols):
                total = landed[c, part]
                for r in range(1, rows):
                    total = total + landed[r * cols + lax.rem((cols - offset) * r + c, cols), part]
                totals.append(total)
            t_high, t_low = split(jnp.concatenate(totals, axis=0))
            both = jnp.dot(jnp.concatenate([t_high, t_low], axis=0), shear[slot], preferred_element_type=jnp.float32)
            line = both[:cols * slices] + both[cols * slices:]
            line = line - jnp.concatenate([measure_in[c, slot] for c in range(cols)], axis=0)
            for c in range(cols):
                resid[c, slot] = line[c * slices:(c + 1) * slices]
            l_high, l_low = split(line)
            both = lax.dot_general(
                jnp.concatenate([l_high, l_low], axis=0), shear[slot], (((1,), (1,)), ((), ())),
                preferred_element_type=jnp.float32)
            spread = both[:cols * slices] + both[cols * slices:]
            for c in range(cols):
                spreads[slot, c] = spread[c * slices:(c + 1) * slices]
            for r in range(rows):
                for c in range(cols):
                    pulls[r * cols + c, slot] = spreads[slot, lax.rem(offset * r + c, cols)]

        others(lambda index, place: send(
            pulls.at[index], pulled.at[pl.ds(mine * per, per)], back_out_sem, back_in_sem, place))
        slot = lax.rem(mine, own_homes) * per

        def send_resid(c):
            @pl.when(jnp.logical_not(jnp.logical_and(owner == row, c == col)))
            def _():
                send(resid.at[c], resid_in.at[pl.ds(slot, per)], r_out_sem, r_in_sem, (owner, c))

        each(cols, send_resid)
        pulled[pl.ds(mine * per, per)] = pulls[me]

        @pl.when(owner == row)
        def _():
            resid_in[pl.ds(slot, per)] = resid[col]

        bytes_of(pulled, angles - per, back_in_sem).wait()

    @pl.when(away)
    def _():
        bytes_of(pulled, angles, back_in_sem).wait()

    for s in range(slices):
        g_high, g_low = split(pulled[:, s, :])
        spread_ref[s] = jnp.concatenate([g_high, g_high, g_low], axis=0)

    @pl.when(owner_here)
    def _():
        bytes_of(resid_in, owned - per, r_in_sem).wait()
        bytes_of(measured, owned - per, m_out_sem).wait()
        bytes_of(resid, cols - 1, r_out_sem).wait()

    @pl.when(jnp.logical_not(owner_here))
    def _():
        bytes_of(resid_in, owned, r_in_sem).wait()
        bytes_of(measured, owned, m_out_sem).wait()

    @pl.when(owner_there)
    def _():
        bytes_of(resid, cols, r_out_sem).wait()

    @pl.when(at_home)
    def _():
        bytes_of(tiles, (homes.count - 1) * block, out_sem).wait()
        bytes_of(pulls, count - 1, back_out_sem).wait()

    @pl.when(away)
    def _():
        bytes_of(tiles, homes.count * block, out_sem).wait()

    residual_ref[...] = resid_in[...]


def finish(columns_ref, spread_ref, resid_ref, residual_ref, gradient_ref, stage, stage_sem, resid_sem):
    copies = [pltpu.make_async_copy(resid_ref, residual_ref, resid_sem)]
    copies[0].start()
    for s in range(spread_ref.shape[0]):
        stage[s] = jnp.dot(columns_ref[...], spread_ref[s], preferred_element_type=jnp.float32)
        copy = pltpu.make_async_copy(stage.at[s], gradient_ref.at[s], stage_sem.at[s])
        copy.start()
        copies.append(copy)
    for copy in copies:
        copy.wait()


def on_device(volume, ray_weights, shear_weights, shear_offsets, measured):
    rows, cols = lax.axis_size("row"), lax.axis_size("col")
    slices, slab_rows, width = volume.shape
    angles = ray_weights.shape[0]
    owned = measured.shape[0]
    count = rows * cols
    homes = Homes(rows, cols, angles)
    per = homes.per
    f32, bf16 = jnp.float32, jnp.bfloat16
    dma = pltpu.SemaphoreType.DMA
    vmem = pl.BlockSpec(memory_space=pltpu.VMEM)
    hbm = pl.BlockSpec(memory_space=pltpu.HBM)

    def blocks(*number):
        return pltpu.VMEM((*number, slices, width), f32)

    columns, spread, resid = pl.pallas_call(
        functools.partial(exchange, rows, cols, 1.0 / math.sqrt(slab_rows * rows), homes),
        out_shape=(
            jax.ShapeDtypeStruct((slab_rows, 3 * angles), bf16),
            jax.ShapeDtypeStruct((slices, 3 * angles, width), bf16),
            jax.ShapeDtypeStruct(measured.shape, f32)),
        in_specs=[hbm] * 5,
        out_specs=(vmem, vmem, vmem),
        scratch_shapes=[
            pltpu.VMEM(volume.shape, f32),
            pltpu.VMEM(ray_weights.shape, f32),
            pltpu.VMEM((per, width, width), shear_weights.dtype),
            pltpu.SMEM(shear_offsets.shape, jnp.int32),
            blocks(owned),
            pltpu.VMEM((angles * slices, width), f32),
            pltpu.VMEM((count, per * slices, width), f32),
            blocks(cols, per), blocks(cols, per), blocks(per, cols), blocks(count, per), blocks(angles), blocks(owned),
            dma((slices,)), dma((4,)), dma, dma, dma, dma, dma, dma, dma, dma,
        ],
        compiler_params=pltpu.CompilerParams(collective_id=0, has_side_effects=True, vmem_limit_bytes=KERNEL_VMEM),
        name="exchange",
    )(*(pltpu.with_memory_space_constraint(value, pltpu.HBM)
        for value in (volume, ray_weights, shear_weights, shear_offsets, measured)))
    return pl.pallas_call(
        finish,
        out_shape=(jax.ShapeDtypeStruct(measured.shape, f32), jax.ShapeDtypeStruct(volume.shape, f32)),
        in_specs=[vmem] * 3,
        out_specs=(hbm, hbm),
        scratch_shapes=[pltpu.VMEM(volume.shape, f32), dma((slices,)), dma],
        compiler_params=pltpu.CompilerParams(vmem_limit_bytes=KERNEL_VMEM),
        name="finish",
    )(columns, spread, resid)


def solution(mesh):
    placed = (P(None, "row", "col"), P(None, "row"), P(), P(), P("row", None, "col"))
    return jax.shard_map(
        on_device,
        mesh=mesh,
        in_specs=placed,
        out_specs=(P("row", None, "col"), P(None, "row", "col")),
        check_vma=False,
    )
```

```python
import functools
import math

import jax
import jax.numpy as jnp
from jax import lax
from jax.experimental import pallas as pl
from jax.experimental.pallas import tpu as pltpu
from jax.sharding import PartitionSpec as P

MESH = pl.DeviceIdType.MESH
UNROLL_UP_TO = 64
KERNEL_VMEM = 24 * 1024 * 1024
LATE_COLUMNS = 8
CHUNK = 2
GROUP = 4


def split(value):
    high = value.astype(jnp.bfloat16)
    return high, (value - high.astype(jnp.float32)).astype(jnp.bfloat16)


def each(count, body):
    if count <= UNROLL_UP_TO:
        for step in range(count):
            body(step)
    else:
        lax.fori_loop(0, count, lambda step, _: (body(step), 0)[1], 0)


def bytes_of(ref, blocks, sem):
    part = ref.at[pl.ds(0, blocks)]
    return pltpu.make_async_copy(part, part, sem)


class Homes:
    def __init__(self, rows, cols, angles):
        self.owned = angles // rows
        self.per = 2 if self.owned % 2 == 0 else 1
        self.count = angles // self.per
        pair = 2 if rows % 2 == 0 and self.count < rows * cols // 2 else 1

        def far(place):
            group, half, deep = place[0] // pair, place[1] % 2, place[1] // 2
            return 10 * group + 10 * half + 11 * deep + 15 * group * half

        devices = [(row, col) for row in range(pair - 1, rows, pair) for col in range(cols)]
        devices.sort(key=lambda place: (far(place), place))
        skipped = 1 if self.count < len(devices) else 0
        self.places = sorted(devices[skipped:skipped + self.count])
        self.order = sorted(range(self.count), key=lambda home: (self.places[home][1] // 2, home))

    def owner(self, home):
        return home * self.per // self.owned


def wrap(index, size):
    return lax.rem(index, size) if size & (size - 1) else jnp.bitwise_and(index, size - 1)


def pick(later, first, second):
    return tuple(lax.select(later, jnp.int32(after), jnp.int32(before)) for before, after in zip(first, second))


def exchange(
    rows, cols, factor, homes,
    volume_ref, weights_ref, shear_ref, offsets_ref, measured_ref,
    columns_ref, pulled, resid_in,
    slab, weights_in, shear, turned, offsets, measured, tiles, landed, measure_in, resid, spreads, pulls,
    slab_sem, local_sem, out_sem, in_sem, back_out_sem, back_in_sem, m_out_sem, m_in_sem, r_out_sem, r_in_sem,
):
    slices = volume_ref.shape[0]
    angles = weights_ref.shape[0]
    owned = measured_ref.shape[0]
    width = volume_ref.shape[2]
    per = homes.per
    own_homes = owned // per
    count = rows * cols
    row, col = lax.axis_index("row"), lax.axis_index("col")
    me = row * cols + col
    hits = [me == place[0] * cols + place[1] for place in homes.places]
    at_home = functools.reduce(jnp.logical_or, hits)
    away = jnp.logical_not(at_home)
    mine = sum(hit.astype(jnp.int32) * home for home, hit in enumerate(hits))
    owner = homes.owner(mine)
    owner_here = jnp.logical_and(at_home, owner == row)
    owner_there = jnp.logical_and(at_home, owner != row)
    late = col >= cols - cols // LATE_COLUMNS

    def others(body, start=0, stop=count - 1, last_first=False):
        rank = col * rows + row

        def at(step):
            step = count - 2 - step if last_first else step
            index = step + (step >= rank).astype(jnp.int32)
            body(lax.rem(index, rows) * cols + index // rows, (lax.rem(index, rows), index // rows))

        if count <= UNROLL_UP_TO:
            for step in range(start, stop):
                at(step)
        else:
            lax.fori_loop(start, stop, lambda step, carry: (at(step), carry)[1], 0)

    def send(source, target, send_sem, recv_sem, place):
        pltpu.make_async_remote_copy(
            src_ref=source, dst_ref=target, send_sem=send_sem, recv_sem=recv_sem,
            device_id=place, device_id_type=MESH).start()

    block = per * slices
    barrier = pltpu.get_barrier_semaphore()

    weights_copy = pltpu.make_async_copy(weights_ref, weights_in, local_sem.at[0])
    weights_copy.start()
    measured_copy = pltpu.make_async_copy(measured_ref, measured, local_sem.at[2])
    measured_copy.start()
    volume_copies = []
    for s in range(0, slices, CHUNK):
        copy = pltpu.make_async_copy(volume_ref.at[pl.ds(s, CHUNK)], slab.at[pl.ds(s, CHUNK)], slab_sem.at[s])
        copy.start()
        volume_copies.append(copy)

    @pl.when(at_home)
    def _():
        others(lambda index, place: pl.semaphore_signal(barrier, inc=1, device_id=place, device_id_type=MESH),
               last_first=True)

    shear_copy = pltpu.make_async_copy(shear_ref.at[pl.ds(mine * per, per)], shear, local_sem.at[1])
    shear_copy.start()
    offsets_copy = pltpu.make_async_copy(offsets_ref, offsets, local_sem.at[3])
    offsets_copy.start()

    def meet():
        @pl.when(at_home)
        def _():
            pl.semaphore_wait(barrier, homes.count - 1)

        @pl.when(away)
        def _():
            pl.semaphore_wait(barrier, homes.count)

    def send_measured():
        measured_copy.wait()
        for r in range(rows):
            @pl.when(row == r)
            def _():
                for k in range(own_homes):
                    place = homes.places[r * own_homes + k]
                    if place[0] != r:
                        send(measured.at[pl.ds(k * per, per)], measure_in.at[col], m_out_sem, m_in_sem, place)
                        continue

                    @pl.when(col != place[1])
                    def _():
                        send(measured.at[pl.ds(k * per, per)], measure_in.at[col], m_out_sem, m_in_sem, place)

                    @pl.when(col == place[1])
                    def _():
                        measure_in[col] = measured[k * per:(k + 1) * per]

    @pl.when(late)
    def _():
        meet()
        send_measured()

    weights_copy.wait()
    weights = weights_in[...] * factor
    w_high, w_low = split(weights)
    w_both = jnp.concatenate([w_high, w_low], axis=0)
    for s in range(0, slices, GROUP):
        for copy in volume_copies[s // CHUNK:(s + GROUP) // CHUNK]:
            copy.wait()
        v_high, v_low = split(jnp.concatenate([slab[s + i] for i in range(GROUP)], axis=1))
        first = jnp.dot(w_both, v_high, preferred_element_type=jnp.float32)
        second = jnp.dot(w_high, v_low, preferred_element_type=jnp.float32)
        total = first[:angles] + first[angles:] + second
        for i in range(GROUP):
            tiles[pl.ds(s + i, angles, stride=slices), :] = total[:, i * width:(i + 1) * width]

    pl.when(jnp.logical_not(late))(meet)

    order = homes.order
    rank = sum((mine == home).astype(jnp.int32) * turn for turn, home in enumerate(order))
    rank = lax.select(at_home, rank, jnp.int32(homes.count))

    def send_tile(turn):
        before, after = order[turn], order[min(turn + 1, homes.count - 1)]
        home, *place = pick(turn >= rank, (before, *homes.places[before]), (after, *homes.places[after]))
        source = tiles.at[pl.ds(pl.multiple_of(home * block, block), block)]
        send(source, landed.at[me], out_sem, in_sem, tuple(place))

    for turn in range(homes.count - 1):
        send_tile(turn)
    pl.when(away)(functools.partial(send_tile, homes.count - 1))
    pl.when(jnp.logical_not(late))(send_measured)
    shear_copy.wait()
    offsets_copy.wait()

    columns_ref[...] = jnp.concatenate(
        [weights, weights - w_high.astype(jnp.float32), weights], axis=0).T.astype(jnp.bfloat16)

    @pl.when(at_home)
    def _():
        landed[me] = tiles[pl.ds(pl.multiple_of(mine * block, block), block), :]
        for slot in range(per):
            turned[slot] = shear[slot].T

    @pl.when(owner_here)
    def _():
        bytes_of(measured, owned - per, m_out_sem).wait()

    @pl.when(jnp.logical_not(owner_here))
    def _():
        bytes_of(measured, owned, m_out_sem).wait()

    @pl.when(owner_here)
    def _():
        bytes_of(measure_in, cols - 1, m_in_sem).wait()

    @pl.when(owner_there)
    def _():
        bytes_of(measure_in, cols, m_in_sem).wait()

    @pl.when(at_home)
    def _():
        first = lax.rem(mine, own_homes) * per
        owned_here = owner == row

        def send_pull(index, place):
            send(pulls.at[index], pulled.at[pl.ds(mine * per, per)], back_out_sem, back_in_sem, place)

        def send_resid(step):
            c = wrap(col + step, cols)
            send(resid.at[c], resid_in.at[pl.ds(first, per)], r_out_sem, r_in_sem, (owner, c))

        shifts = [[wrap(offsets[mine * per + slot] * r, cols) for r in range(rows)] for slot in range(per)]
        bytes_of(landed, count - 1, in_sem).wait()
        lines = []
        for slot in range(per):
            part = slice(slot * slices, (slot + 1) * slices)
            totals = []
            for c in range(cols):
                total = landed[c, part]
                for r in range(1, rows):
                    total = total + landed[r * cols + wrap(cols - shifts[slot][r] + c, cols), part]
                totals.append(total)
            both = jnp.concatenate(split(jnp.concatenate(totals, axis=0)), axis=1)
            twice = jnp.concatenate([shear[slot]] * 2, axis=0)
            line = jnp.dot(both, twice, preferred_element_type=jnp.float32)
            line = line - jnp.concatenate([measure_in[c, slot] for c in range(cols)], axis=0)
            for c in range(cols):
                resid[c, slot] = line[c * slices:(c + 1) * slices]
            lines.append(line)
        for slot in range(per):
            both = jnp.concatenate(split(lines[slot]), axis=1)
            twice = jnp.concatenate([turned[slot]] * 2, axis=0)
            spread = jnp.dot(both, twice, preferred_element_type=jnp.float32)
            for c in range(cols):
                spreads[slot, c] = spread[c * slices:(c + 1) * slices]
            for r in range(rows):
                for c in range(cols):
                    pulls[r * cols + c, slot] = spreads[slot, wrap(shifts[slot][r] + c, cols)]
        others(send_pull, stop=rows)
        each(cols - 1, lambda step: send_resid(step + 1))
        pl.when(jnp.logical_not(owned_here))(functools.partial(send_resid, 0))
        others(send_pull, start=rows)
        pulled[pl.ds(mine * per, per)] = pulls[me]

        @pl.when(owned_here)
        def _():
            resid_in[pl.ds(first, per)] = resid[col]

        bytes_of(tiles, (homes.count - 1) * block, out_sem).wait()
        bytes_of(pulled, angles - per, back_in_sem).wait()

    @pl.when(away)
    def _():
        bytes_of(tiles, homes.count * block, out_sem).wait()
        bytes_of(pulled, angles, back_in_sem).wait()

    @pl.when(owner_here)
    def _():
        bytes_of(resid_in, owned - per, r_in_sem).wait()
        bytes_of(resid, cols - 1, r_out_sem).wait()

    @pl.when(jnp.logical_not(owner_here))
    def _():
        bytes_of(resid_in, owned, r_in_sem).wait()

    @pl.when(owner_there)
    def _():
        bytes_of(resid, cols, r_out_sem).wait()

    @pl.when(at_home)
    def _():
        bytes_of(pulls, count - 1, back_out_sem).wait()


def finish(columns_ref, pulled_ref, resid_ref, residual_ref, gradient_ref, stage, stage_sem, resid_sem):
    copies = [pltpu.make_async_copy(resid_ref, residual_ref, resid_sem)]
    copies[0].start()
    for s in range(pulled_ref.shape[1]):
        high, low = split(pulled_ref[:, s, :])
        spread = jnp.concatenate([high, high, low], axis=0)
        stage[s] = jnp.dot(columns_ref[...], spread, preferred_element_type=jnp.float32)
        copy = pltpu.make_async_copy(stage.at[s], gradient_ref.at[s], stage_sem.at[s])
        copy.start()
        copies.append(copy)
    for copy in copies:
        copy.wait()


def on_device(volume, ray_weights, shear_weights, shear_offsets, measured):
    rows, cols = lax.axis_size("row"), lax.axis_size("col")
    slices, slab_rows, width = volume.shape
    angles = ray_weights.shape[0]
    owned = measured.shape[0]
    count = rows * cols
    homes = Homes(rows, cols, angles)
    per = homes.per
    f32, bf16 = jnp.float32, jnp.bfloat16
    dma = pltpu.SemaphoreType.DMA
    vmem = pl.BlockSpec(memory_space=pltpu.VMEM)
    hbm = pl.BlockSpec(memory_space=pltpu.HBM)

    def blocks(*number):
        return pltpu.VMEM((*number, slices, width), f32)

    columns, pulled, resid = pl.pallas_call(
        functools.partial(exchange, rows, cols, 1.0 / math.sqrt(slab_rows * rows), homes),
        out_shape=(
            jax.ShapeDtypeStruct((slab_rows, 3 * angles), bf16),
            jax.ShapeDtypeStruct((angles, slices, width), f32),
            jax.ShapeDtypeStruct(measured.shape, f32)),
        in_specs=[hbm] * 5,
        out_specs=(vmem, vmem, vmem),
        scratch_shapes=[
            pltpu.VMEM(volume.shape, f32),
            pltpu.VMEM(ray_weights.shape, f32),
            pltpu.VMEM((per, width, width), shear_weights.dtype),
            pltpu.VMEM((per, width, width), shear_weights.dtype),
            pltpu.SMEM(shear_offsets.shape, jnp.int32),
            blocks(owned),
            pltpu.VMEM((angles * slices, width), f32),
            pltpu.VMEM((count, per * slices, width), f32),
            blocks(cols, per), blocks(cols, per), blocks(per, cols), blocks(count, per),
            dma((slices,)), dma((4,)), dma, dma, dma, dma, dma, dma, dma, dma,
        ],
        compiler_params=pltpu.CompilerParams(collective_id=0, has_side_effects=True, vmem_limit_bytes=KERNEL_VMEM),
        name="exchange",
    )(*(pltpu.with_memory_space_constraint(value, pltpu.HBM)
        for value in (volume, ray_weights, shear_weights, shear_offsets, measured)))
    return pl.pallas_call(
        finish,
        out_shape=(jax.ShapeDtypeStruct(measured.shape, f32), jax.ShapeDtypeStruct(volume.shape, f32)),
        in_specs=[vmem] * 3,
        out_specs=(hbm, hbm),
        scratch_shapes=[pltpu.VMEM(volume.shape, f32), dma((slices,)), dma],
        compiler_params=pltpu.CompilerParams(vmem_limit_bytes=KERNEL_VMEM),
        name="finish",
    )(columns, pulled, resid)


def solution(mesh):
    placed = (P(None, "row", "col"), P(None, "row"), P(), P(), P("row", None, "col"))
    return jax.shard_map(
        on_device,
        mesh=mesh,
        in_specs=placed,
        out_specs=(P("row", None, "col"), P(None, "row", "col")),
        check_vma=False,
    )
```

```python
import functools
import math

import jax
import jax.numpy as jnp
from jax import lax
from jax.experimental import pallas as pl
from jax.experimental.pallas import tpu as pltpu
from jax.sharding import PartitionSpec as P

MESH = pl.DeviceIdType.MESH
UNROLL_UP_TO = 64
KERNEL_VMEM = 24 * 1024 * 1024
LATE_COLUMNS = 4
HALVES = 2


def split(value):
    high = value.astype(jnp.bfloat16)
    return high, (value - high.astype(jnp.float32)).astype(jnp.bfloat16)


def each(count, body):
    if count <= UNROLL_UP_TO:
        for step in range(count):
            body(step)
    else:
        lax.fori_loop(0, count, lambda step, _: (body(step), 0)[1], 0)


def bytes_of(ref, blocks, sem):
    part = ref.at[pl.ds(0, blocks)]
    return pltpu.make_async_copy(part, part, sem)


class Homes:
    def __init__(self, rows, cols, angles):
        self.owned = angles // rows
        self.per = 2 if self.owned % 2 == 0 else 1
        self.count = angles // self.per
        pair = 2 if rows % 2 == 0 and self.count < rows * cols // 2 else 1

        def far(place):
            group, half, deep = place[0] // pair, place[1] % 2, place[1] // 2
            return 10 * group + 10 * half + 11 * deep + 15 * group * half

        devices = [(row, col) for row in range(pair - 1, rows, pair) for col in range(cols)]
        devices.sort(key=lambda place: (far(place), place))
        skipped = 1 if self.count < len(devices) else 0
        self.places = sorted(devices[skipped:skipped + self.count])
        self.order = sorted(range(self.count), key=lambda home: (self.places[home][1] // 2, home))

    def owner(self, home):
        return home * self.per // self.owned


def wrap(index, size):
    return lax.rem(index, size) if size & (size - 1) else jnp.bitwise_and(index, size - 1)


def pick(later, first, second):
    return tuple(lax.select(later, jnp.int32(after), jnp.int32(before)) for before, after in zip(first, second))


def exchange(
    rows, cols, factor, homes,
    volume_ref, weights_ref, shear_ref, offsets_ref, measured_ref,
    columns_ref, pulled, resid_in,
    slab, weights_in, shear, gains, offsets, measured, leaving, tiles, landed, measure_in, resid, spreads, pulls,
    slab_sem, local_sem, out_sem, in_sem, back_in_sem, m_out_sem, m_in_sem, r_in_sem,
):
    slices = volume_ref.shape[0]
    angles = weights_ref.shape[0]
    owned = measured_ref.shape[0]
    width = volume_ref.shape[2]
    per = homes.per
    own_homes = owned // per
    count = rows * cols
    row, col = lax.axis_index("row"), lax.axis_index("col")
    me = row * cols + col
    hits = [me == place[0] * cols + place[1] for place in homes.places]
    at_home = functools.reduce(jnp.logical_or, hits)
    away = jnp.logical_not(at_home)
    mine = sum(hit.astype(jnp.int32) * home for home, hit in enumerate(hits))
    owner = homes.owner(mine)
    owner_here = jnp.logical_and(at_home, owner == row)
    owner_there = jnp.logical_and(at_home, owner != row)
    late = col >= cols - cols // LATE_COLUMNS

    def others(body, start=0, stop=count - 1, last_first=False):
        rank = col * rows + row

        def at(step):
            step = count - 2 - step if last_first else step
            index = step + (step >= rank).astype(jnp.int32)
            body(lax.rem(index, rows) * cols + index // rows, (lax.rem(index, rows), index // rows))

        if count <= UNROLL_UP_TO:
            for step in range(start, stop):
                at(step)
        else:
            lax.fori_loop(start, stop, lambda step, carry: (at(step), carry)[1], 0)

    def send(source, target, send_sem, recv_sem, place):
        pltpu.make_async_remote_copy(
            src_ref=source, dst_ref=target, send_sem=send_sem, recv_sem=recv_sem,
            device_id=place, device_id_type=MESH).start()

    group = slices // HALVES
    block = per * group
    barrier = pltpu.get_barrier_semaphore()

    weights_copy = pltpu.make_async_copy(weights_ref, weights_in, local_sem.at[0])
    weights_copy.start()
    measured_copy = pltpu.make_async_copy(measured_ref, measured, local_sem.at[1])
    measured_copy.start()
    volume_copies = []
    for half in range(HALVES):
        part = pl.ds(half * group, group)
        copy = pltpu.make_async_copy(volume_ref.at[part], slab.at[part], slab_sem.at[half])
        copy.start()
        volume_copies.append(copy)

    @pl.when(at_home)
    def _():
        others(lambda index, place: pl.semaphore_signal(barrier, inc=1, device_id=place, device_id_type=MESH),
               last_first=True)

    def meet():
        @pl.when(at_home)
        def _():
            pl.semaphore_wait(barrier, homes.count - 1)

        @pl.when(away)
        def _():
            pl.semaphore_wait(barrier, homes.count)

    def send_measured():
        measured_copy.wait()
        for s in range(slices):
            leaving[s // group, pl.ds(s % group, owned, stride=group), :] = measured[:, s, :]
        for r in range(rows):
            @pl.when(row == r)
            def _():
                for k in range(own_homes):
                    place = homes.places[r * own_homes + k]
                    source = leaving.at[:, pl.ds(k * block, block)]
                    if place[0] != r:
                        send(source, measure_in.at[col], m_out_sem, m_in_sem, place)
                        continue

                    @pl.when(col != place[1])
                    def _():
                        send(source, measure_in.at[col], m_out_sem, m_in_sem, place)

                    @pl.when(col == place[1])
                    def _():
                        measure_in[col] = leaving[:, k * block:(k + 1) * block]

    @pl.when(late)
    def _():
        meet()
        send_measured()

    weights_copy.wait()
    weights = weights_in[...] * factor
    w_high, w_low = split(weights)
    w_both = jnp.concatenate([w_high, w_low], axis=0)
    def send_tiles(halves):
        order = homes.order
        rank = sum((mine == home).astype(jnp.int32) * turn for turn, home in enumerate(order))
        rank = lax.select(at_home, rank, jnp.int32(homes.count))

        def send_tile(half, turn):
            before, after = order[turn], order[min(turn + 1, homes.count - 1)]
            home, *place = pick(turn >= rank, (before, *homes.places[before]), (after, *homes.places[after]))
            source = tiles.at[half, pl.ds(pl.multiple_of(home * block, block), block)]
            send(source, landed.at[me, half], out_sem, in_sem, tuple(place))

        for half in halves:
            for turn in range(homes.count - 1):
                send_tile(half, turn)

        @pl.when(away)
        def _():
            for half in halves:
                send_tile(half, homes.count - 1)

    for half in range(HALVES):
        volume_copies[half].wait()
        v_high, v_low = split(jnp.concatenate([slab[half * group + i] for i in range(group)], axis=1))
        first = jnp.dot(w_both, v_high, preferred_element_type=jnp.float32)
        second = jnp.dot(w_high, v_low, preferred_element_type=jnp.float32)
        total = first[:angles] + first[angles:] + second
        for i in range(group):
            tiles[half, pl.ds(i, angles, stride=group), :] = total[:, i * width:(i + 1) * width]
        if half < HALVES - 1:
            pl.when(late)(functools.partial(send_tiles, [half]))

    @pl.when(late)
    def _():
        send_tiles([HALVES - 1])

    @pl.when(jnp.logical_not(late))
    def _():
        meet()
        send_tiles(range(HALVES))

    pl.when(jnp.logical_not(late))(send_measured)
    shear_copy = pltpu.make_async_copy(shear_ref.at[pl.ds(mine * per, per)], shear, local_sem.at[0])
    shear_copy.start()
    offsets_copy = pltpu.make_async_copy(offsets_ref, offsets, local_sem.at[1])
    offsets_copy.start()

    columns_ref[...] = jnp.concatenate(
        [weights, weights - w_high.astype(jnp.float32), weights], axis=0).T.astype(jnp.bfloat16)

    @pl.when(at_home)
    def _():
        landed[me] = tiles[:, pl.ds(pl.multiple_of(mine * block, block), block), :]
    shear_copy.wait()
    offsets_copy.wait()

    @pl.when(at_home)
    def _():
        for slot in range(per):
            part = slice(slot * width, (slot + 1) * width)
            square = lax.dot_general(
                shear[slot], shear[slot], (((1,), (1,)), ((), ())), preferred_element_type=jnp.float32)
            gains[0, :, part], gains[1, :, part] = split(square)
            gains[2, :, part] = shear[slot]
            gains[3, :, part] = shear[slot].T

    @pl.when(at_home)
    def _():
        bytes_of(pulls, homes.count - 1, out_sem).wait()

    @pl.when(away)
    def _():
        bytes_of(pulls, homes.count, out_sem).wait()

    @pl.when(owner_here)
    def _():
        bytes_of(measure_in, own_homes - 1, m_out_sem).wait()

    @pl.when(jnp.logical_not(owner_here))
    def _():
        bytes_of(measure_in, own_homes, m_out_sem).wait()

    @pl.when(owner_here)
    def _():
        bytes_of(measure_in, cols - 1, m_in_sem).wait()

    @pl.when(owner_there)
    def _():
        bytes_of(measure_in, cols, m_in_sem).wait()

    @pl.when(at_home)
    def _():
        first = pl.ds(pl.multiple_of(lax.rem(mine, own_homes) * block, block), block)
        here = pl.ds(pl.multiple_of(mine * block, block), block)
        owned_here = owner == row

        def send_pull(index, place):
            send(pulls.at[index], pulled.at[:, here], out_sem, back_in_sem, place)

        def send_resid(step):
            c = step + (step >= lax.select(owned_here, col, jnp.int32(cols))).astype(jnp.int32)
            send(resid.at[c], resid_in.at[:, first], m_out_sem, r_in_sem, (owner, c))

        def by_slot(parts):
            chosen = parts[0]
            for slot in range(1, per):
                chosen = jnp.where(slot_of[:chosen.shape[0]] >= slot, parts[slot], chosen)
            return chosen

        def times(high, low, right, rest=None):
            product = jnp.dot(jnp.concatenate([high, low], axis=1), jnp.concatenate([right] * 2, axis=0),
                              preferred_element_type=jnp.float32)
            if rest is not None:
                product = product + jnp.dot(high, rest, preferred_element_type=jnp.float32)
            return by_slot([product[:, slot * width:(slot + 1) * width] for slot in range(per)])

        height = HALVES * cols * block
        slot_of = lax.rem(lax.broadcasted_iota(jnp.int32, (height, width), 0), block) // group
        shifts = [[wrap(offsets[mine * per + slot] * r, cols) for r in range(rows)] for slot in range(per)]
        bytes_of(landed, count - 1, in_sem).wait()
        totals = []
        for c in range(cols):
            sources = [[wrap(cols - shifts[slot][r] + c, cols) for slot in range(per)] for r in range(rows)]
            for half in range(HALVES):
                total = landed[c, half]
                for r in range(1, rows):
                    total = total + by_slot([landed[r * cols + sources[r][slot], half] for slot in range(per)])
                totals.append(total)
        t_high, t_low = split(jnp.concatenate(totals, axis=0))
        level = jnp.concatenate([measure_in[c, half] for c in range(cols) for half in range(HALVES)], axis=0)
        spread = times(t_high, t_low, gains[0], gains[1]) - times(*split(level), gains[3])
        line = times(t_high, t_low, gains[2]) - level
        for c in range(cols):
            for half in range(HALVES):
                at = (c * HALVES + half) * block
                resid[c, half] = line[at:at + block]
        for c in range(cols):
            for half in range(HALVES):
                at = (c * HALVES + half) * block
                spreads[c, half] = spread[at:at + block]
        for c in range(cols):
            for half in range(HALVES):
                pulls[c, half] = spreads[c, half]
        for r in range(1, rows):
            for c in range(cols):
                sources = [wrap(shifts[slot][r] + c, cols) for slot in range(per)]
                for half in range(HALVES):
                    pulls[r * cols + c, half] = by_slot([spreads[source, half] for source in sources])
        others(send_pull, stop=2)
        send_resid(0)
        others(send_pull, start=2, stop=3 * rows)
        each(cols - 2, lambda step: send_resid(step + 1))
        pl.when(jnp.logical_not(owned_here))(functools.partial(send_resid, cols - 1))
        others(send_pull, start=3 * rows)
        pulled[:, here] = pulls[me]

        @pl.when(owned_here)
        def _():
            resid_in[:, first] = resid[col]

        bytes_of(pulls, homes.count - 1, back_in_sem).wait()

    @pl.when(away)
    def _():
        bytes_of(pulls, homes.count, back_in_sem).wait()

    @pl.when(owner_here)
    def _():
        bytes_of(resid, own_homes - 1, r_in_sem).wait()
        bytes_of(resid, cols - 1, m_out_sem).wait()

    @pl.when(jnp.logical_not(owner_here))
    def _():
        bytes_of(resid, own_homes, r_in_sem).wait()

    @pl.when(owner_there)
    def _():
        bytes_of(resid, cols, m_out_sem).wait()

    @pl.when(at_home)
    def _():
        bytes_of(pulls, count - 1, out_sem).wait()


def finish(columns_ref, pulled_ref, resid_ref, residual_ref, gradient_ref, stage, natural, stage_sem, resid_sem):
    owned, slices, width = natural.shape
    group = slices // HALVES
    angles = pulled_ref.shape[1] // group
    for s in range(slices):
        high, low = split(pulled_ref[s // group, pl.ds(s % group, angles, stride=group), :])
        spread = jnp.concatenate([high, high, low], axis=0)
        stage[s] = jnp.dot(columns_ref[...], spread, preferred_element_type=jnp.float32)
        pltpu.make_async_copy(stage.at[s], gradient_ref.at[s], stage_sem).start()
        natural[:, s, :] = resid_ref[s // group, pl.ds(s % group, owned, stride=group), :]
    copy = pltpu.make_async_copy(natural, residual_ref, resid_sem)
    copy.start()
    pltpu.make_async_copy(stage, gradient_ref, stage_sem).wait()
    copy.wait()


def on_device(volume, ray_weights, shear_weights, shear_offsets, measured):
    rows, cols = lax.axis_size("row"), lax.axis_size("col")
    slices, slab_rows, width = volume.shape
    angles = ray_weights.shape[0]
    owned = measured.shape[0]
    count = rows * cols
    homes = Homes(rows, cols, angles)
    per = homes.per
    f32, bf16 = jnp.float32, jnp.bfloat16
    dma = pltpu.SemaphoreType.DMA
    vmem = pl.BlockSpec(memory_space=pltpu.VMEM)
    hbm = pl.BlockSpec(memory_space=pltpu.HBM)

    group = slices // HALVES

    def halves(*number):
        return pltpu.VMEM((*number, HALVES, per * group, width), f32)

    columns, pulled, resid = pl.pallas_call(
        functools.partial(exchange, rows, cols, 1.0 / math.sqrt(slab_rows * rows), homes),
        out_shape=(
            jax.ShapeDtypeStruct((slab_rows, 3 * angles), bf16),
            jax.ShapeDtypeStruct((HALVES, angles * group, width), f32),
            jax.ShapeDtypeStruct((HALVES, owned * group, width), f32)),
        in_specs=[hbm] * 5,
        out_specs=(vmem, vmem, vmem),
        scratch_shapes=[
            pltpu.VMEM(volume.shape, f32),
            pltpu.VMEM(ray_weights.shape, f32),
            pltpu.VMEM((per, width, width), shear_weights.dtype),
            pltpu.VMEM((4, width, per * width), shear_weights.dtype),
            pltpu.SMEM(shear_offsets.shape, jnp.int32),
            pltpu.VMEM(measured.shape, f32),
            pltpu.VMEM((HALVES, owned * group, width), f32),
            pltpu.VMEM((HALVES, angles * group, width), f32),
            halves(count), halves(cols), halves(cols), halves(cols), halves(count),
            dma((HALVES,)), dma((2,)), dma, dma, dma, dma, dma, dma,
        ],
        compiler_params=pltpu.CompilerParams(collective_id=0, has_side_effects=True, vmem_limit_bytes=KERNEL_VMEM),
        name="exchange",
    )(*(pltpu.with_memory_space_constraint(value, pltpu.HBM)
        for value in (volume, ray_weights, shear_weights, shear_offsets, measured)))
    return pl.pallas_call(
        finish,
        out_shape=(jax.ShapeDtypeStruct(measured.shape, f32), jax.ShapeDtypeStruct(volume.shape, f32)),
        in_specs=[vmem] * 3,
        out_specs=(hbm, hbm),
        scratch_shapes=[pltpu.VMEM(volume.shape, f32), pltpu.VMEM(measured.shape, f32), dma, dma],
        compiler_params=pltpu.CompilerParams(vmem_limit_bytes=KERNEL_VMEM),
        name="finish",
    )(columns, pulled, resid)


def solution(mesh):
    placed = (P(None, "row", "col"), P(None, "row"), P(), P(), P("row", None, "col"))
    return jax.shard_map(
        on_device,
        mesh=mesh,
        in_specs=placed,
        out_specs=(P("row", None, "col"), P(None, "row", "col")),
        check_vma=False,
    )
```

```python
import functools
import math

import jax
import jax.numpy as jnp
from jax import lax
from jax.experimental import pallas as pl
from jax.experimental.pallas import tpu as pltpu
from jax.sharding import PartitionSpec as P

MESH = pl.DeviceIdType.MESH
UNROLL_UP_TO = 64
KERNEL_VMEM = 24 * 1024 * 1024
LATE_COLUMNS = 4
HALVES = 2
CHUNKS = 2


def split(value):
    high = value.astype(jnp.bfloat16)
    return high, (value - high.astype(jnp.float32)).astype(jnp.bfloat16)


def each(count, body):
    if count <= UNROLL_UP_TO:
        for step in range(count):
            body(step)
    else:
        lax.fori_loop(0, count, lambda step, _: (body(step), 0)[1], 0)


def bytes_of(ref, blocks, sem):
    part = ref.at[pl.ds(0, blocks)]
    return pltpu.make_async_copy(part, part, sem)


class Homes:
    def __init__(self, rows, cols, angles):
        self.owned = angles // rows
        self.per = 2 if self.owned % 2 == 0 else 1
        self.count = angles // self.per
        pair = 2 if rows % 2 == 0 and self.count < rows * cols // 2 else 1

        def far(place):
            group, half, deep = place[0] // pair, place[1] % 2, place[1] // 2
            return 10 * group + 10 * half + 11 * deep + 15 * group * half

        devices = [(row, col) for row in range(pair - 1, rows, pair) for col in range(cols)]
        devices.sort(key=lambda place: (far(place), place))
        skipped = 1 if self.count < len(devices) else 0
        self.places = sorted(devices[skipped:skipped + self.count])
        self.order = sorted(range(self.count), key=lambda home: (self.places[home][1] // 2, home))

    def owner(self, home):
        return home * self.per // self.owned


def wrap(index, size):
    return lax.rem(index, size) if size & (size - 1) else jnp.bitwise_and(index, size - 1)


def pick(later, first, second):
    return tuple(lax.select(later, jnp.int32(after), jnp.int32(before)) for before, after in zip(first, second))


def exchange(
    rows, cols, factor, homes,
    volume_ref, weights_ref, shear_ref, offsets_ref, measured_ref,
    columns_ref, pulled, resid_in,
    slab, weights_in, shear, gains, offsets, measured, leaving, tiles, landed, measure_in, resid, spreads, pulls,
    slab_sem, local_sem, out_sem, in_sem, back_in_sem, m_out_sem, m_in_sem, r_in_sem,
):
    slices = volume_ref.shape[0]
    angles = weights_ref.shape[0]
    owned = measured_ref.shape[0]
    width = volume_ref.shape[2]
    per = homes.per
    own_homes = owned // per
    count = rows * cols
    row, col = lax.axis_index("row"), lax.axis_index("col")
    me = row * cols + col
    hits = [me == place[0] * cols + place[1] for place in homes.places]
    at_home = functools.reduce(jnp.logical_or, hits)
    away = jnp.logical_not(at_home)
    mine = sum(hit.astype(jnp.int32) * home for home, hit in enumerate(hits))
    owner = homes.owner(mine)
    owner_here = jnp.logical_and(at_home, owner == row)
    owner_there = jnp.logical_and(at_home, owner != row)
    late = col >= cols - cols // LATE_COLUMNS

    def others(body, start=0, stop=count - 1, last_first=False):
        rank = col * rows + row

        def at(step):
            step = count - 2 - step if last_first else step
            index = step + (step >= rank).astype(jnp.int32)
            body(lax.rem(index, rows) * cols + index // rows, (lax.rem(index, rows), index // rows))

        if count <= UNROLL_UP_TO:
            for step in range(start, stop):
                at(step)
        else:
            lax.fori_loop(start, stop, lambda step, carry: (at(step), carry)[1], 0)

    def send(source, target, send_sem, recv_sem, place):
        pltpu.make_async_remote_copy(
            src_ref=source, dst_ref=target, send_sem=send_sem, recv_sem=recv_sem,
            device_id=place, device_id_type=MESH).start()

    group = slices // HALVES
    block = per * group
    barrier = pltpu.get_barrier_semaphore()

    weights_copy = pltpu.make_async_copy(weights_ref, weights_in, local_sem.at[0])
    weights_copy.start()
    measured_copy = pltpu.make_async_copy(measured_ref, measured, local_sem.at[1])
    measured_copy.start()
    for chunk in range(HALVES * CHUNKS):
        part = pl.ds(chunk * (group // CHUNKS), group // CHUNKS)
        pltpu.make_async_copy(volume_ref.at[part], slab.at[part], slab_sem.at[chunk // CHUNKS]).start()

    @pl.when(at_home)
    def _():
        def greet(index, place):
            pl.semaphore_signal(barrier, inc=1, device_id=place, device_id_type=MESH)

        others(greet, stop=2 * rows)
        others(greet, stop=count - 1 - 2 * rows, last_first=True)

    def meet():
        @pl.when(at_home)
        def _():
            pl.semaphore_wait(barrier, homes.count - 1)

        @pl.when(away)
        def _():
            pl.semaphore_wait(barrier, homes.count)

    def send_measured():
        measured_copy.wait()
        for s in range(slices):
            leaving[s // group, pl.ds(s % group, owned, stride=group), :] = measured[:, s, :]
        for r in range(rows):
            @pl.when(row == r)
            def _():
                for k in range(own_homes):
                    place = homes.places[r * own_homes + k]
                    source = leaving.at[:, pl.ds(k * block, block)]
                    if place[0] != r:
                        send(source, measure_in.at[col], m_out_sem, m_in_sem, place)
                        continue

                    @pl.when(col != place[1])
                    def _():
                        send(source, measure_in.at[col], m_out_sem, m_in_sem, place)

                    @pl.when(col == place[1])
                    def _():
                        measure_in[col] = leaving[:, k * block:(k + 1) * block]

    @pl.when(late)
    def _():
        meet()
        send_measured()

    weights_copy.wait()
    weights = weights_in[...] * factor
    w_high, w_low = split(weights)
    w_both = jnp.concatenate([w_high, w_low], axis=0)
    def send_tiles(halves, order=homes.order):
        rank = sum((mine == home).astype(jnp.int32) * turn for turn, home in enumerate(order))
        rank = lax.select(at_home, rank, jnp.int32(homes.count))

        def send_tile(half, turn):
            before, after = order[turn], order[min(turn + 1, homes.count - 1)]
            home, *place = pick(turn >= rank, (before, *homes.places[before]), (after, *homes.places[after]))
            source = tiles.at[half, pl.ds(pl.multiple_of(home * block, block), block)]
            send(source, landed.at[me, half], out_sem, in_sem, tuple(place))

        for half in halves:
            for turn in range(homes.count - 1):
                send_tile(half, turn)

        @pl.when(away)
        def _():
            for half in halves:
                send_tile(half, homes.count - 1)

    for half in range(HALVES):
        part = pl.ds(half * group, group)
        pltpu.make_async_copy(volume_ref.at[part], slab.at[part], slab_sem.at[half]).wait()
        v_high, v_low = split(jnp.concatenate([slab[half * group + i] for i in range(group)], axis=1))
        first = jnp.dot(w_both, v_high, preferred_element_type=jnp.float32)
        second = jnp.dot(w_high, v_low, preferred_element_type=jnp.float32)
        total = first[:angles] + first[angles:] + second
        for i in range(group):
            tiles[half, pl.ds(i, angles, stride=group), :] = total[:, i * width:(i + 1) * width]
        if half < HALVES - 1:
            pl.when(late)(functools.partial(send_tiles, [half]))

    @pl.when(late)
    def _():
        send_tiles([HALVES - 1])

    @pl.when(jnp.logical_not(late))
    def _():
        meet()
        send_tiles(range(HALVES), homes.order[::-1])

    pl.when(jnp.logical_not(late))(send_measured)
    shear_copy = pltpu.make_async_copy(shear_ref.at[pl.ds(mine * per, per)], shear, local_sem.at[0])
    shear_copy.start()
    offsets_copy = pltpu.make_async_copy(offsets_ref, offsets, local_sem.at[1])
    offsets_copy.start()

    columns_ref[...] = jnp.concatenate(
        [weights, weights - w_high.astype(jnp.float32), weights], axis=0).T.astype(jnp.bfloat16)

    @pl.when(at_home)
    def _():
        landed[me] = tiles[:, pl.ds(pl.multiple_of(mine * block, block), block), :]
    shear_copy.wait()
    offsets_copy.wait()

    @pl.when(at_home)
    def _():
        for slot in range(per):
            part = slice(slot * width, (slot + 1) * width)
            square = lax.dot_general(
                shear[slot], shear[slot], (((1,), (1,)), ((), ())), preferred_element_type=jnp.float32)
            gains[0, :, part], gains[1, :, part] = split(square)
            gains[2, :, part] = shear[slot]
            gains[3, :, part] = shear[slot].T

    @pl.when(at_home)
    def _():
        bytes_of(pulls, homes.count - 1, out_sem).wait()

    @pl.when(away)
    def _():
        bytes_of(pulls, homes.count, out_sem).wait()

    @pl.when(owner_here)
    def _():
        bytes_of(measure_in, own_homes - 1, m_out_sem).wait()

    @pl.when(jnp.logical_not(owner_here))
    def _():
        bytes_of(measure_in, own_homes, m_out_sem).wait()

    @pl.when(owner_here)
    def _():
        bytes_of(measure_in, cols - 1, m_in_sem).wait()

    @pl.when(owner_there)
    def _():
        bytes_of(measure_in, cols, m_in_sem).wait()

    @pl.when(at_home)
    def _():
        first = pl.ds(pl.multiple_of(lax.rem(mine, own_homes) * block, block), block)
        here = pl.ds(pl.multiple_of(mine * block, block), block)
        owned_here = owner == row

        def send_pull(index, place):
            send(pulls.at[index], pulled.at[:, here], out_sem, back_in_sem, place)

        def send_resid(step):
            c = step + (step >= lax.select(owned_here, col, jnp.int32(cols))).astype(jnp.int32)
            send(resid.at[c], resid_in.at[:, first], m_out_sem, r_in_sem, (owner, c))

        def by_slot(parts):
            chosen = parts[0]
            for slot in range(1, per):
                chosen = jnp.where(slot_of[:chosen.shape[0]] >= slot, parts[slot], chosen)
            return chosen

        def times(high, low, right, rest=None):
            product = jnp.dot(jnp.concatenate([high, low], axis=1), jnp.concatenate([right] * 2, axis=0),
                              preferred_element_type=jnp.float32)
            if rest is not None:
                product = product + jnp.dot(high, rest, preferred_element_type=jnp.float32)
            return by_slot([product[:, slot * width:(slot + 1) * width] for slot in range(per)])

        height = HALVES * cols * block
        slot_of = lax.rem(lax.broadcasted_iota(jnp.int32, (height, width), 0), block) // group
        shifts = [[wrap(offsets[mine * per + slot] * r, cols) for r in range(rows)] for slot in range(per)]
        bytes_of(landed, count - 1, in_sem).wait()
        totals = []
        for c in range(cols):
            sources = [[wrap(cols - shifts[slot][r] + c, cols) for slot in range(per)] for r in range(rows)]
            for half in range(HALVES):
                total = landed[c, half]
                for r in range(1, rows):
                    total = total + by_slot([landed[r * cols + sources[r][slot], half] for slot in range(per)])
                totals.append(total)
        t_high, t_low = split(jnp.concatenate(totals, axis=0))
        level = jnp.concatenate([measure_in[c, half] for c in range(cols) for half in range(HALVES)], axis=0)
        spread = times(t_high, t_low, gains[0], gains[1]) - times(*split(level), gains[3])
        line = times(t_high, t_low, gains[2]) - level
        tile = [[slice((c * HALVES + half) * block, (c * HALVES + half + 1) * block) for half in range(HALVES)]
                for c in range(cols)]

        def lay_pulls(c, rows_of):
            for r in rows_of:
                sources = [wrap(shifts[slot][r] + c, cols) for slot in range(per)]
                for half in range(HALVES):
                    pulls[r * cols + c, half] = by_slot([spreads[source, half] for source in sources])

        for c in range(cols):
            for half in range(HALVES):
                spreads[c, half] = spread[tile[c][half]]
        for half in range(HALVES):
            pulls[0, half] = spread[tile[0][half]]
        lay_pulls(0, range(1, rows))
        early = min(2, rows - 1)
        others(send_pull, stop=early)
        for c in range(cols):
            for half in range(HALVES):
                resid[c, half] = line[tile[c][half]]
        for c in range(1, cols):
            for half in range(HALVES):
                pulls[c, half] = spread[tile[c][half]]
        for c in range(1, cols):
            lay_pulls(c, range(1, rows))
        send_resid(0)
        others(send_pull, start=early, stop=3 * rows)
        each(cols - 2, lambda step: send_resid(step + 1))
        pl.when(jnp.logical_not(owned_here))(functools.partial(send_resid, cols - 1))
        others(send_pull, start=3 * rows)
        pulled[:, here] = pulls[me]

        @pl.when(owned_here)
        def _():
            resid_in[:, first] = resid[col]

        bytes_of(pulls, homes.count - 1, back_in_sem).wait()

    @pl.when(away)
    def _():
        bytes_of(pulls, homes.count, back_in_sem).wait()

    @pl.when(owner_here)
    def _():
        bytes_of(resid, own_homes - 1, r_in_sem).wait()
        bytes_of(resid, cols - 1, m_out_sem).wait()

    @pl.when(jnp.logical_not(owner_here))
    def _():
        bytes_of(resid, own_homes, r_in_sem).wait()

    @pl.when(owner_there)
    def _():
        bytes_of(resid, cols, m_out_sem).wait()

    @pl.when(at_home)
    def _():
        bytes_of(pulls, count - 1, out_sem).wait()


def finish(columns_ref, pulled_ref, resid_ref, residual_ref, gradient_ref, stage, natural, stage_sem, resid_sem):
    owned, slices, width = natural.shape
    group = slices // HALVES
    angles = pulled_ref.shape[1] // group
    for s in range(slices):
        high, low = split(pulled_ref[s // group, pl.ds(s % group, angles, stride=group), :])
        spread = jnp.concatenate([high, high, low], axis=0)
        stage[s] = jnp.dot(columns_ref[...], spread, preferred_element_type=jnp.float32)
        pltpu.make_async_copy(stage.at[s], gradient_ref.at[s], stage_sem).start()
        natural[:, s, :] = resid_ref[s // group, pl.ds(s % group, owned, stride=group), :]
    copy = pltpu.make_async_copy(natural, residual_ref, resid_sem)
    copy.start()
    pltpu.make_async_copy(stage, gradient_ref, stage_sem).wait()
    copy.wait()


def on_device(volume, ray_weights, shear_weights, shear_offsets, measured):
    rows, cols = lax.axis_size("row"), lax.axis_size("col")
    slices, slab_rows, width = volume.shape
    angles = ray_weights.shape[0]
    owned = measured.shape[0]
    count = rows * cols
    homes = Homes(rows, cols, angles)
    per = homes.per
    f32, bf16 = jnp.float32, jnp.bfloat16
    dma = pltpu.SemaphoreType.DMA
    vmem = pl.BlockSpec(memory_space=pltpu.VMEM)
    hbm = pl.BlockSpec(memory_space=pltpu.HBM)

    group = slices // HALVES

    def halves(*number):
        return pltpu.VMEM((*number, HALVES, per * group, width), f32)

    columns, pulled, resid = pl.pallas_call(
        functools.partial(exchange, rows, cols, 1.0 / math.sqrt(slab_rows * rows), homes),
        out_shape=(
            jax.ShapeDtypeStruct((slab_rows, 3 * angles), bf16),
            jax.ShapeDtypeStruct((HALVES, angles * group, width), f32),
            jax.ShapeDtypeStruct((HALVES, owned * group, width), f32)),
        in_specs=[hbm] * 5,
        out_specs=(vmem, vmem, vmem),
        scratch_shapes=[
            pltpu.VMEM(volume.shape, f32),
            pltpu.VMEM(ray_weights.shape, f32),
            pltpu.VMEM((per, width, width), shear_weights.dtype),
            pltpu.VMEM((4, width, per * width), shear_weights.dtype),
            pltpu.SMEM(shear_offsets.shape, jnp.int32),
            pltpu.VMEM(measured.shape, f32),
            pltpu.VMEM((HALVES, owned * group, width), f32),
            pltpu.VMEM((HALVES, angles * group, width), f32),
            halves(count), halves(cols), halves(cols), halves(cols), halves(count),
            dma((HALVES,)), dma((2,)), dma, dma, dma, dma, dma, dma,
        ],
        compiler_params=pltpu.CompilerParams(collective_id=0, has_side_effects=True, vmem_limit_bytes=KERNEL_VMEM),
        name="exchange",
    )(*(pltpu.with_memory_space_constraint(value, pltpu.HBM)
        for value in (volume, ray_weights, shear_weights, shear_offsets, measured)))
    return pl.pallas_call(
        finish,
        out_shape=(jax.ShapeDtypeStruct(measured.shape, f32), jax.ShapeDtypeStruct(volume.shape, f32)),
        in_specs=[vmem] * 3,
        out_specs=(hbm, hbm),
        scratch_shapes=[pltpu.VMEM(volume.shape, f32), pltpu.VMEM(measured.shape, f32), dma, dma],
        compiler_params=pltpu.CompilerParams(vmem_limit_bytes=KERNEL_VMEM),
        name="finish",
    )(columns, pulled, resid)


def solution(mesh):
    placed = (P(None, "row", "col"), P(None, "row"), P(), P(), P("row", None, "col"))
    return jax.shard_map(
        on_device,
        mesh=mesh,
        in_specs=placed,
        out_specs=(P("row", None, "col"), P(None, "row", "col")),
        check_vma=False,
    )
```

```python
import functools
import math

import jax
import jax.numpy as jnp
from jax import lax
from jax.experimental import pallas as pl
from jax.experimental.pallas import tpu as pltpu
from jax.sharding import PartitionSpec as P

MESH = pl.DeviceIdType.MESH
UNROLL_UP_TO = 64
KERNEL_VMEM = 24 * 1024 * 1024
LATE_COLUMNS = 4
HALVES = 2
CHUNKS = 2


def split(value):
    high = value.astype(jnp.bfloat16)
    return high, (value - high.astype(jnp.float32)).astype(jnp.bfloat16)


def each(count, body):
    if count <= UNROLL_UP_TO:
        for step in range(count):
            body(step)
    else:
        lax.fori_loop(0, count, lambda step, _: (body(step), 0)[1], 0)


def bytes_of(ref, blocks, sem):
    part = ref.at[pl.ds(0, blocks)]
    return pltpu.make_async_copy(part, part, sem)


class Homes:
    def __init__(self, rows, cols, angles):
        self.owned = angles // rows
        self.per = 2 if self.owned % 2 == 0 else 1
        self.count = angles // self.per
        pair = 2 if rows % 2 == 0 and self.count < rows * cols // 2 else 1

        def far(place):
            group, half, deep = place[0] // pair, place[1] % 2, place[1] // 2
            return 10 * group + 10 * half + 11 * deep + 15 * group * half

        devices = [(row, col) for row in range(pair - 1, rows, pair) for col in range(cols)]
        devices.sort(key=lambda place: (far(place), place))
        skipped = 1 if self.count < len(devices) else 0
        self.places = sorted(devices[skipped:skipped + self.count])
        self.order = sorted(range(self.count), key=lambda home: (self.places[home][1] // 2, home))

    def owner(self, home):
        return home * self.per // self.owned


def wrap(index, size):
    return lax.rem(index, size) if size & (size - 1) else jnp.bitwise_and(index, size - 1)


def pick(later, first, second):
    return tuple(lax.select(later, jnp.int32(after), jnp.int32(before)) for before, after in zip(first, second))


def exchange(
    rows, cols, factor, homes,
    volume_ref, weights_ref, shear_ref, offsets_ref, measured_ref,
    columns_ref, pulled, resid_in,
    slab, weights_in, shear, gains, offsets, measured, leaving, tiles, landed, measure_in, resid, spreads, pulls,
    slab_sem, out_sem, in_sem, back_in_sem, m_out_sem, m_in_sem, r_in_sem,
):
    slices = volume_ref.shape[0]
    angles = weights_ref.shape[0]
    owned = measured_ref.shape[0]
    width = volume_ref.shape[2]
    per = homes.per
    own_homes = owned // per
    count = rows * cols
    row, col = lax.axis_index("row"), lax.axis_index("col")
    me = row * cols + col
    hits = [me == place[0] * cols + place[1] for place in homes.places]
    at_home = functools.reduce(jnp.logical_or, hits)
    away = jnp.logical_not(at_home)
    mine = sum(hit.astype(jnp.int32) * home for home, hit in enumerate(hits))
    owner = homes.owner(mine)
    owner_here = jnp.logical_and(at_home, owner == row)
    owner_there = jnp.logical_and(at_home, owner != row)
    late = col >= cols - cols // LATE_COLUMNS

    def others(body, start=0, stop=count - 1, last_first=False):
        rank = col * rows + row

        def at(step):
            step = count - 2 - step if last_first else step
            index = step + (step >= rank).astype(jnp.int32)
            body(lax.rem(index, rows) * cols + index // rows, (lax.rem(index, rows), index // rows))

        if count <= UNROLL_UP_TO:
            for step in range(start, stop):
                at(step)
        else:
            lax.fori_loop(start, stop, lambda step, carry: (at(step), carry)[1], 0)

    def send(source, target, send_sem, recv_sem, place):
        pltpu.make_async_remote_copy(
            src_ref=source, dst_ref=target, send_sem=send_sem, recv_sem=recv_sem,
            device_id=place, device_id_type=MESH).start()

    group = slices // HALVES
    block = per * group
    barrier = pltpu.get_barrier_semaphore()

    weights_copy = pltpu.make_async_copy(weights_ref, weights_in, out_sem)
    weights_copy.start()
    measured_copy = pltpu.make_async_copy(measured_ref, measured, m_out_sem)
    measured_copy.start()
    for chunk in range(HALVES * CHUNKS):
        part = pl.ds(chunk * (group // CHUNKS), group // CHUNKS)
        pltpu.make_async_copy(volume_ref.at[part], slab.at[part], slab_sem.at[chunk // CHUNKS]).start()

    @pl.when(at_home)
    def _():
        def greet(index, place):
            pl.semaphore_signal(barrier, inc=1, device_id=place, device_id_type=MESH)

        others(greet, stop=2 * rows)
        others(greet, stop=count - 1 - 2 * rows, last_first=True)

    def meet():
        @pl.when(at_home)
        def _():
            pl.semaphore_wait(barrier, homes.count - 1)

        @pl.when(away)
        def _():
            pl.semaphore_wait(barrier, homes.count)

    def send_measured():
        measured_copy.wait()
        for s in range(slices):
            leaving[s // group, pl.ds(s % group, owned, stride=group), :] = measured[:, s, :]
        for r in range(rows):
            @pl.when(row == r)
            def _():
                for k in range(own_homes):
                    place = homes.places[r * own_homes + k]
                    source = leaving.at[:, pl.ds(k * block, block)]
                    if place[0] != r:
                        send(source, measure_in.at[col], m_out_sem, m_in_sem, place)
                        continue

                    @pl.when(col != place[1])
                    def _():
                        send(source, measure_in.at[col], m_out_sem, m_in_sem, place)

                    @pl.when(col == place[1])
                    def _():
                        measure_in[col] = leaving[:, k * block:(k + 1) * block]

    @pl.when(late)
    def _():
        meet()
        send_measured()

    weights_copy.wait()
    weights = weights_in[...] * factor
    w_high, w_low = split(weights)
    w_both = jnp.concatenate([w_high, w_low], axis=0)
    def send_tiles(halves, order=homes.order):
        rank = sum((mine == home).astype(jnp.int32) * turn for turn, home in enumerate(order))
        rank = lax.select(at_home, rank, jnp.int32(homes.count))

        def send_tile(half, turn):
            before, after = order[turn], order[min(turn + 1, homes.count - 1)]
            home, *place = pick(turn >= rank, (before, *homes.places[before]), (after, *homes.places[after]))
            source = tiles.at[half, pl.ds(pl.multiple_of(home * block, block), block)]
            send(source, landed.at[me, half], out_sem, in_sem, tuple(place))

        for half in halves:
            for turn in range(homes.count - 1):
                send_tile(half, turn)

        @pl.when(away)
        def _():
            for half in halves:
                send_tile(half, homes.count - 1)

    for half in range(HALVES):
        part = pl.ds(half * group, group)
        pltpu.make_async_copy(volume_ref.at[part], slab.at[part], slab_sem.at[half]).wait()
        v_high, v_low = split(jnp.concatenate([slab[half * group + i] for i in range(group)], axis=1))
        first = jnp.dot(w_both, v_high, preferred_element_type=jnp.float32)
        second = jnp.dot(w_high, v_low, preferred_element_type=jnp.float32)
        total = first[:angles] + first[angles:] + second
        for i in range(group):
            tiles[half, pl.ds(i, angles, stride=group), :] = total[:, i * width:(i + 1) * width]
        if half < HALVES - 1:
            pl.when(late)(functools.partial(send_tiles, [half]))

    @pl.when(late)
    def _():
        send_tiles([HALVES - 1])

    @pl.when(jnp.logical_not(late))
    def _():
        meet()
        send_tiles(range(HALVES), homes.order[::-1])

    pl.when(jnp.logical_not(late))(send_measured)
    shear_copy = pltpu.make_async_copy(shear_ref.at[pl.ds(mine * per, per)], shear, slab_sem.at[0])
    shear_copy.start()
    offsets_copy = pltpu.make_async_copy(offsets_ref, offsets, slab_sem.at[1])
    offsets_copy.start()

    columns_ref[...] = jnp.concatenate(
        [weights, weights - w_high.astype(jnp.float32), weights], axis=0).T.astype(jnp.bfloat16)

    @pl.when(at_home)
    def _():
        landed[me] = tiles[:, pl.ds(pl.multiple_of(mine * block, block), block), :]
    shear_copy.wait()
    offsets_copy.wait()

    @pl.when(at_home)
    def _():
        for slot in range(per):
            part = slice(slot * width, (slot + 1) * width)
            square = lax.dot_general(
                shear[slot], shear[slot], (((1,), (1,)), ((), ())), preferred_element_type=jnp.float32)
            gains[0, :, part], gains[1, :, part] = split(square)
            gains[2, :, part] = shear[slot]
            gains[3, :, part] = shear[slot].T

    @pl.when(at_home)
    def _():
        bytes_of(pulls, homes.count - 1, out_sem).wait()

    @pl.when(away)
    def _():
        bytes_of(pulls, homes.count, out_sem).wait()

    @pl.when(owner_here)
    def _():
        bytes_of(measure_in, own_homes - 1, m_out_sem).wait()

    @pl.when(jnp.logical_not(owner_here))
    def _():
        bytes_of(measure_in, own_homes, m_out_sem).wait()

    @pl.when(owner_here)
    def _():
        bytes_of(measure_in, cols - 1, m_in_sem).wait()

    @pl.when(owner_there)
    def _():
        bytes_of(measure_in, cols, m_in_sem).wait()

    @pl.when(at_home)
    def _():
        first = pl.ds(pl.multiple_of(lax.rem(mine, own_homes) * block, block), block)
        here = pl.ds(pl.multiple_of(mine * block, block), block)
        owned_here = owner == row

        def send_pull(index, place):
            send(pulls.at[index], pulled.at[:, here], out_sem, back_in_sem, place)

        def send_resid(step):
            c = step + (step >= lax.select(owned_here, col, jnp.int32(cols))).astype(jnp.int32)
            send(resid.at[c], resid_in.at[:, first], m_out_sem, r_in_sem, (owner, c))

        def by_slot(parts):
            chosen = parts[0]
            for slot in range(1, per):
                chosen = jnp.where(slot_of[:chosen.shape[0]] >= slot, parts[slot], chosen)
            return chosen

        def times(high, low, right, rest=None):
            product = jnp.dot(jnp.concatenate([high, low], axis=1), jnp.concatenate([right] * 2, axis=0),
                              preferred_element_type=jnp.float32)
            if rest is not None:
                product = product + jnp.dot(high, rest, preferred_element_type=jnp.float32)
            return by_slot([product[:, slot * width:(slot + 1) * width] for slot in range(per)])

        height = HALVES * cols * block
        slot_of = lax.rem(lax.broadcasted_iota(jnp.int32, (height, width), 0), block) // group
        shifts = [[wrap(offsets[mine * per + slot] * r, cols) for r in range(rows)] for slot in range(per)]
        bytes_of(landed, count - 1, in_sem).wait()
        totals = []
        for c in range(cols):
            sources = [[wrap(cols - shifts[slot][r] + c, cols) for slot in range(per)] for r in range(rows)]
            for half in range(HALVES):
                total = landed[c, half]
                for r in range(1, rows):
                    total = total + by_slot([landed[r * cols + sources[r][slot], half] for slot in range(per)])
                totals.append(total)
        t_high, t_low = split(jnp.concatenate(totals, axis=0))
        level = jnp.concatenate([measure_in[c, half] for c in range(cols) for half in range(HALVES)], axis=0)
        spread = times(t_high, t_low, gains[0], gains[1]) - times(*split(level), gains[3])
        line = times(t_high, t_low, gains[2]) - level
        tile = [[slice((c * HALVES + half) * block, (c * HALVES + half + 1) * block) for half in range(HALVES)]
                for c in range(cols)]

        def lay_pulls(c, rows_of):
            for r in rows_of:
                sources = [wrap(shifts[slot][r] + c, cols) for slot in range(per)]
                for half in range(HALVES):
                    pulls[r * cols + c, half] = by_slot([spreads[source, half] for source in sources])

        for c in range(cols):
            for half in range(HALVES):
                spreads[c, half] = spread[tile[c][half]]
        for half in range(HALVES):
            pulls[0, half] = spread[tile[0][half]]
        lay_pulls(0, range(1, rows))
        early = min(2, rows - 1)
        others(send_pull, stop=early)
        for c in range(cols):
            for half in range(HALVES):
                resid[c, half] = line[tile[c][half]]
        for c in range(1, cols):
            for half in range(HALVES):
                pulls[c, half] = spread[tile[c][half]]
        for c in range(1, cols):
            lay_pulls(c, range(1, rows))
        send_resid(0)
        others(send_pull, start=early, stop=3 * rows)
        each(cols - 2, lambda step: send_resid(step + 1))
        pl.when(jnp.logical_not(owned_here))(functools.partial(send_resid, cols - 1))
        others(send_pull, start=3 * rows)
        pulled[:, here] = pulls[me]

        @pl.when(owned_here)
        def _():
            resid_in[:, first] = resid[col]

        bytes_of(pulls, homes.count - 1, back_in_sem).wait()

    @pl.when(away)
    def _():
        bytes_of(pulls, homes.count, back_in_sem).wait()

    @pl.when(owner_here)
    def _():
        bytes_of(resid, own_homes - 1, r_in_sem).wait()
        bytes_of(resid, cols - 1, m_out_sem).wait()

    @pl.when(jnp.logical_not(owner_here))
    def _():
        bytes_of(resid, own_homes, r_in_sem).wait()

    @pl.when(owner_there)
    def _():
        bytes_of(resid, cols, m_out_sem).wait()

    @pl.when(at_home)
    def _():
        bytes_of(pulls, count - 1, out_sem).wait()


def finish(columns_ref, pulled_ref, resid_ref, residual_ref, gradient_ref, stage, natural, stage_sem, resid_sem):
    owned, slices, width = natural.shape
    group = slices // HALVES
    angles = pulled_ref.shape[1] // group
    for s in range(slices):
        high, low = split(pulled_ref[s // group, pl.ds(s % group, angles, stride=group), :])
        spread = jnp.concatenate([high, high, low], axis=0)
        stage[s] = jnp.dot(columns_ref[...], spread, preferred_element_type=jnp.float32)
        pltpu.make_async_copy(stage.at[s], gradient_ref.at[s], stage_sem).start()
        natural[:, s, :] = resid_ref[s // group, pl.ds(s % group, owned, stride=group), :]
    copy = pltpu.make_async_copy(natural, residual_ref, resid_sem)
    copy.start()
    pltpu.make_async_copy(stage, gradient_ref, stage_sem).wait()
    copy.wait()


def on_device(volume, ray_weights, shear_weights, shear_offsets, measured):
    rows, cols = lax.axis_size("row"), lax.axis_size("col")
    slices, slab_rows, width = volume.shape
    angles = ray_weights.shape[0]
    owned = measured.shape[0]
    count = rows * cols
    homes = Homes(rows, cols, angles)
    per = homes.per
    f32, bf16 = jnp.float32, jnp.bfloat16
    dma = pltpu.SemaphoreType.DMA
    vmem = pl.BlockSpec(memory_space=pltpu.VMEM)
    hbm = pl.BlockSpec(memory_space=pltpu.HBM)

    group = slices // HALVES

    def halves(*number):
        return pltpu.VMEM((*number, HALVES, per * group, width), f32)

    columns, pulled, resid = pl.pallas_call(
        functools.partial(exchange, rows, cols, 1.0 / math.sqrt(slab_rows * rows), homes),
        out_shape=(
            jax.ShapeDtypeStruct((slab_rows, 3 * angles), bf16),
            jax.ShapeDtypeStruct((HALVES, angles * group, width), f32),
            jax.ShapeDtypeStruct((HALVES, owned * group, width), f32)),
        in_specs=[hbm] * 5,
        out_specs=(vmem, vmem, vmem),
        scratch_shapes=[
            pltpu.VMEM(volume.shape, f32),
            pltpu.VMEM(ray_weights.shape, f32),
            pltpu.VMEM((per, width, width), shear_weights.dtype),
            pltpu.VMEM((4, width, per * width), shear_weights.dtype),
            pltpu.SMEM(shear_offsets.shape, jnp.int32),
            pltpu.VMEM(measured.shape, f32),
            pltpu.VMEM((HALVES, owned * group, width), f32),
            pltpu.VMEM((HALVES, angles * group, width), f32),
            halves(count), halves(cols), halves(cols), halves(cols), halves(count),
            dma((HALVES,)), dma, dma, dma, dma, dma, dma,
        ],
        compiler_params=pltpu.CompilerParams(collective_id=0, has_side_effects=True, vmem_limit_bytes=KERNEL_VMEM),
        name="exchange",
    )(*(pltpu.with_memory_space_constraint(value, pltpu.HBM)
        for value in (volume, ray_weights, shear_weights, shear_offsets, measured)))
    return pl.pallas_call(
        finish,
        out_shape=(jax.ShapeDtypeStruct(measured.shape, f32), jax.ShapeDtypeStruct(volume.shape, f32)),
        in_specs=[vmem] * 3,
        out_specs=(hbm, hbm),
        scratch_shapes=[pltpu.VMEM(volume.shape, f32), pltpu.VMEM(measured.shape, f32), dma, dma],
        compiler_params=pltpu.CompilerParams(vmem_limit_bytes=KERNEL_VMEM),
        name="finish",
    )(columns, pulled, resid)


def solution(mesh):
    placed = (P(None, "row", "col"), P(None, "row"), P(), P(), P("row", None, "col"))
    return jax.shard_map(
        on_device,
        mesh=mesh,
        in_specs=placed,
        out_specs=(P("row", None, "col"), P(None, "row", "col")),
        check_vma=False,
    )
```

```python
import functools
import math

import jax
import jax.numpy as jnp
from jax import lax
from jax.experimental import pallas as pl
from jax.experimental.pallas import tpu as pltpu
from jax.sharding import PartitionSpec as P

MESH = pl.DeviceIdType.MESH
UNROLL_UP_TO = 64
KERNEL_VMEM = 24 * 1024 * 1024
LATE_COLUMNS = 4
HALVES = 2
CHUNKS = 2


def split(value):
    high = value.astype(jnp.bfloat16)
    return high, (value - high.astype(jnp.float32)).astype(jnp.bfloat16)


def each(count, body):
    if count <= UNROLL_UP_TO:
        for step in range(count):
            body(step)
    else:
        lax.fori_loop(0, count, lambda step, _: (body(step), 0)[1], 0)


def bytes_of(ref, blocks, sem):
    part = ref.at[pl.ds(0, blocks)]
    return pltpu.make_async_copy(part, part, sem)


class Homes:
    def __init__(self, rows, cols, angles):
        self.owned = angles // rows
        self.per = 2 if self.owned % 2 == 0 else 1
        self.count = angles // self.per
        pair = 2 if rows % 2 == 0 and self.count < rows * cols // 2 else 1

        def far(place):
            group, half, deep = place[0] // pair, place[1] % 2, place[1] // 2
            return 10 * group + 10 * half + 11 * deep + 15 * group * half

        devices = [(row, col) for row in range(pair - 1, rows, pair) for col in range(cols)]
        devices.sort(key=lambda place: (far(place), place))
        skipped = 1 if self.count < len(devices) else 0
        self.places = sorted(devices[skipped:skipped + self.count])
        self.order = sorted(range(self.count), key=lambda home: (self.places[home][1] // 2, home))

    def owner(self, home):
        return home * self.per // self.owned


def wrap(index, size):
    return lax.rem(index, size) if size & (size - 1) else jnp.bitwise_and(index, size - 1)


def pick(later, first, second):
    return tuple(lax.select(later, jnp.int32(after), jnp.int32(before)) for before, after in zip(first, second))


def exchange(
    rows, cols, factor, homes,
    volume_ref, weights_ref, shear_ref, offsets_ref, measured_ref,
    columns_ref, pulled, resid_in,
    slab, weights_in, shear, gains, offsets, measured, leaving, tiles, landed, resid, spreads, pulls,
    slab_sem, out_sem, in_sem, back_in_sem,
):
    slices = volume_ref.shape[0]
    angles = weights_ref.shape[0]
    owned = measured_ref.shape[0]
    width = volume_ref.shape[2]
    per = homes.per
    own_homes = owned // per
    count = rows * cols
    row, col = lax.axis_index("row"), lax.axis_index("col")
    me = row * cols + col
    hits = [me == place[0] * cols + place[1] for place in homes.places]
    at_home = functools.reduce(jnp.logical_or, hits)
    away = jnp.logical_not(at_home)
    mine = sum(hit.astype(jnp.int32) * home for home, hit in enumerate(hits))
    owner = homes.owner(mine)
    owner_here = jnp.logical_and(at_home, owner == row)
    owner_there = jnp.logical_and(at_home, owner != row)
    late = col >= cols - cols // LATE_COLUMNS

    def others(body, start=0, stop=count - 1, last_first=False):
        rank = col * rows + row

        def at(step):
            step = count - 2 - step if last_first else step
            index = step + (step >= rank).astype(jnp.int32)
            body(lax.rem(index, rows) * cols + index // rows, (lax.rem(index, rows), index // rows))

        if count <= UNROLL_UP_TO:
            for step in range(start, stop):
                at(step)
        else:
            lax.fori_loop(start, stop, lambda step, carry: (at(step), carry)[1], 0)

    def send(source, target, send_sem, recv_sem, place):
        pltpu.make_async_remote_copy(
            src_ref=source, dst_ref=target, send_sem=send_sem, recv_sem=recv_sem,
            device_id=place, device_id_type=MESH).start()

    group = slices // HALVES
    block = per * group
    barrier = pltpu.get_barrier_semaphore()

    weights_copy = pltpu.make_async_copy(weights_ref, weights_in, out_sem)
    weights_copy.start()
    measured_copy = pltpu.make_async_copy(measured_ref, measured, out_sem)
    measured_copy.start()
    for chunk in range(HALVES * CHUNKS):
        part = pl.ds(chunk * (group // CHUNKS), group // CHUNKS)
        pltpu.make_async_copy(volume_ref.at[part], slab.at[part], slab_sem.at[chunk // CHUNKS]).start()

    @pl.when(at_home)
    def _():
        def greet(index, place):
            pl.semaphore_signal(barrier, inc=1, device_id=place, device_id_type=MESH)

        others(greet, stop=2 * rows)
        others(greet, stop=count - 1 - 2 * rows, last_first=True)

    def local_wait():
        size = weights_ref.size + measured_ref.size
        bytes_of(landed, size // (HALVES * block * width), out_sem).wait()

    def meet():
        @pl.when(at_home)
        def _():
            pl.semaphore_wait(barrier, homes.count - 1)

        @pl.when(away)
        def _():
            pl.semaphore_wait(barrier, homes.count)

    def send_measured():
        for s in range(slices):
            leaving[s // group, pl.ds(s % group, owned, stride=group), :] = measured[:, s, :]
        for r in range(rows):
            @pl.when(row == r)
            def _():
                for k in range(own_homes):
                    place = homes.places[r * own_homes + k]
                    source = leaving.at[:, pl.ds(k * block, block)]
                    if place[0] != r:
                        send(source, landed.at[count + col], out_sem, in_sem, place)
                        continue

                    @pl.when(col != place[1])
                    def _():
                        send(source, landed.at[count + col], out_sem, in_sem, place)

                    @pl.when(col == place[1])
                    def _():
                        landed[count + col] = leaving[:, k * block:(k + 1) * block]

    @pl.when(late)
    def _():
        meet()
        local_wait()
        send_measured()

    pl.when(jnp.logical_not(late))(local_wait)
    weights = weights_in[...] * factor
    w_high, w_low = split(weights)
    w_both = jnp.concatenate([w_high, w_low], axis=0)
    def send_tiles(halves, order=homes.order):
        rank = sum((mine == home).astype(jnp.int32) * turn for turn, home in enumerate(order))
        rank = lax.select(at_home, rank, jnp.int32(homes.count))

        def send_tile(half, turn):
            before, after = order[turn], order[min(turn + 1, homes.count - 1)]
            home, *place = pick(turn >= rank, (before, *homes.places[before]), (after, *homes.places[after]))
            source = tiles.at[half, pl.ds(pl.multiple_of(home * block, block), block)]
            send(source, landed.at[me, half], out_sem, in_sem, tuple(place))

        for half in halves:
            for turn in range(homes.count - 1):
                send_tile(half, turn)

        @pl.when(away)
        def _():
            for half in halves:
                send_tile(half, homes.count - 1)

    for half in range(HALVES):
        part = pl.ds(half * group, group)
        pltpu.make_async_copy(volume_ref.at[part], slab.at[part], slab_sem.at[half]).wait()
        v_high, v_low = split(jnp.concatenate([slab[half * group + i] for i in range(group)], axis=1))
        first = jnp.dot(w_both, v_high, preferred_element_type=jnp.float32)
        second = jnp.dot(w_high, v_low, preferred_element_type=jnp.float32)
        total = first[:angles] + first[angles:] + second
        for i in range(group):
            tiles[half, pl.ds(i, angles, stride=group), :] = total[:, i * width:(i + 1) * width]
        if half < HALVES - 1:
            pl.when(late)(functools.partial(send_tiles, [half]))

    @pl.when(late)
    def _():
        send_tiles([HALVES - 1])

    @pl.when(jnp.logical_not(late))
    def _():
        meet()
        send_tiles(range(HALVES), homes.order[::-1])

    pl.when(jnp.logical_not(late))(send_measured)
    shear_copy = pltpu.make_async_copy(shear_ref.at[pl.ds(mine * per, per)], shear, slab_sem.at[0])
    shear_copy.start()
    offsets_copy = pltpu.make_async_copy(offsets_ref, offsets, slab_sem.at[1])
    offsets_copy.start()

    columns_ref[...] = jnp.concatenate(
        [weights, weights - w_high.astype(jnp.float32), weights], axis=0).T.astype(jnp.bfloat16)

    @pl.when(at_home)
    def _():
        landed[me] = tiles[:, pl.ds(pl.multiple_of(mine * block, block), block), :]
    shear_copy.wait()
    offsets_copy.wait()

    @pl.when(at_home)
    def _():
        for slot in range(per):
            part = slice(slot * width, (slot + 1) * width)
            square = lax.dot_general(
                shear[slot], shear[slot], (((1,), (1,)), ((), ())), preferred_element_type=jnp.float32)
            gains[0, :, part], gains[1, :, part] = split(square)
            gains[2, :, part] = shear[slot]
            gains[3, :, part] = shear[slot].T

    def drained(ref, blocks, sem):
        for case, fewer in ((away, 0), (owner_there, 1), (owner_here, 2)):
            pl.when(case)(lambda fewer=fewer: bytes_of(ref, blocks - fewer, sem).wait())

    drained(landed, homes.count + own_homes, out_sem)

    @pl.when(at_home)
    def _():
        first = pl.ds(pl.multiple_of(lax.rem(mine, own_homes) * block, block), block)
        here = pl.ds(pl.multiple_of(mine * block, block), block)
        owned_here = owner == row

        def send_pull(index, place):
            send(pulls.at[index], pulled.at[:, here], out_sem, back_in_sem, place)

        def send_resid(step):
            c = step + (step >= lax.select(owned_here, col, jnp.int32(cols))).astype(jnp.int32)
            send(resid.at[c], resid_in.at[:, first], out_sem, back_in_sem, (owner, c))

        def by_slot(parts):
            chosen = parts[0]
            for slot in range(1, per):
                chosen = jnp.where(slot_of[:chosen.shape[0]] >= slot, parts[slot], chosen)
            return chosen

        def times(high, low, right, rest=None):
            product = jnp.dot(jnp.concatenate([high, low], axis=1), jnp.concatenate([right] * 2, axis=0),
                              preferred_element_type=jnp.float32)
            if rest is not None:
                product = product + jnp.dot(high, rest, preferred_element_type=jnp.float32)
            return by_slot([product[:, slot * width:(slot + 1) * width] for slot in range(per)])

        height = HALVES * cols * block
        slot_of = lax.rem(lax.broadcasted_iota(jnp.int32, (height, width), 0), block) // group
        shifts = [[wrap(offsets[mine * per + slot] * r, cols) for r in range(rows)] for slot in range(per)]
        @pl.when(owned_here)
        def _():
            bytes_of(landed, count - 1 + cols - 1, in_sem).wait()

        @pl.when(jnp.logical_not(owned_here))
        def _():
            bytes_of(landed, count - 1 + cols, in_sem).wait()

        totals = []
        for c in range(cols):
            sources = [[wrap(cols - shifts[slot][r] + c, cols) for slot in range(per)] for r in range(rows)]
            for half in range(HALVES):
                total = landed[c, half]
                for r in range(1, rows):
                    total = total + by_slot([landed[r * cols + sources[r][slot], half] for slot in range(per)])
                totals.append(total)
        t_high, t_low = split(jnp.concatenate(totals, axis=0))
        level = jnp.concatenate([landed[count + c, half] for c in range(cols) for half in range(HALVES)], axis=0)
        spread = times(t_high, t_low, gains[0], gains[1]) - times(*split(level), gains[3])
        line = times(t_high, t_low, gains[2]) - level
        tile = [[slice((c * HALVES + half) * block, (c * HALVES + half + 1) * block) for half in range(HALVES)]
                for c in range(cols)]

        def lay_pulls(c, rows_of):
            for r in rows_of:
                sources = [wrap(shifts[slot][r] + c, cols) for slot in range(per)]
                for half in range(HALVES):
                    pulls[r * cols + c, half] = by_slot([spreads[source, half] for source in sources])

        for c in range(cols):
            for half in range(HALVES):
                spreads[c, half] = spread[tile[c][half]]
        for half in range(HALVES):
            pulls[0, half] = spread[tile[0][half]]
        lay_pulls(0, range(1, rows))
        early = min(2, rows - 1)
        others(send_pull, stop=early)
        for c in range(cols):
            for half in range(HALVES):
                resid[c, half] = line[tile[c][half]]
        for c in range(1, cols):
            for half in range(HALVES):
                pulls[c, half] = spread[tile[c][half]]
        for c in range(1, cols):
            lay_pulls(c, range(1, rows))
        send_resid(0)
        others(send_pull, start=early, stop=3 * rows)
        each(cols - 2, lambda step: send_resid(step + 1))
        pl.when(jnp.logical_not(owned_here))(functools.partial(send_resid, cols - 1))
        others(send_pull, start=3 * rows)
        pulled[:, here] = pulls[me]

        @pl.when(owned_here)
        def _():
            resid_in[:, first] = resid[col]

    drained(landed, homes.count + own_homes, back_in_sem)

    @pl.when(owner_here)
    def _():
        bytes_of(landed, count - 1 + cols - 1, out_sem).wait()

    @pl.when(owner_there)
    def _():
        bytes_of(landed, count - 1 + cols, out_sem).wait()


def finish(columns_ref, pulled_ref, resid_ref, residual_ref, gradient_ref, stage, natural, stage_sem, resid_sem):
    owned, slices, width = natural.shape
    group = slices // HALVES
    angles = pulled_ref.shape[1] // group
    for s in range(slices):
        high, low = split(pulled_ref[s // group, pl.ds(s % group, angles, stride=group), :])
        spread = jnp.concatenate([high, high, low], axis=0)
        stage[s] = jnp.dot(columns_ref[...], spread, preferred_element_type=jnp.float32)
        pltpu.make_async_copy(stage.at[s], gradient_ref.at[s], stage_sem).start()
        natural[:, s, :] = resid_ref[s // group, pl.ds(s % group, owned, stride=group), :]
    copy = pltpu.make_async_copy(natural, residual_ref, resid_sem)
    copy.start()
    pltpu.make_async_copy(stage, gradient_ref, stage_sem).wait()
    copy.wait()


def on_device(volume, ray_weights, shear_weights, shear_offsets, measured):
    rows, cols = lax.axis_size("row"), lax.axis_size("col")
    slices, slab_rows, width = volume.shape
    angles = ray_weights.shape[0]
    owned = measured.shape[0]
    count = rows * cols
    homes = Homes(rows, cols, angles)
    per = homes.per
    f32, bf16 = jnp.float32, jnp.bfloat16
    dma = pltpu.SemaphoreType.DMA
    vmem = pl.BlockSpec(memory_space=pltpu.VMEM)
    hbm = pl.BlockSpec(memory_space=pltpu.HBM)

    group = slices // HALVES

    def halves(*number):
        return pltpu.VMEM((*number, HALVES, per * group, width), f32)

    columns, pulled, resid = pl.pallas_call(
        functools.partial(exchange, rows, cols, 1.0 / math.sqrt(slab_rows * rows), homes),
        out_shape=(
            jax.ShapeDtypeStruct((slab_rows, 3 * angles), bf16),
            jax.ShapeDtypeStruct((HALVES, angles * group, width), f32),
            jax.ShapeDtypeStruct((HALVES, owned * group, width), f32)),
        in_specs=[hbm] * 5,
        out_specs=(vmem, vmem, vmem),
        scratch_shapes=[
            pltpu.VMEM(volume.shape, f32),
            pltpu.VMEM(ray_weights.shape, f32),
            pltpu.VMEM((per, width, width), shear_weights.dtype),
            pltpu.VMEM((4, width, per * width), shear_weights.dtype),
            pltpu.SMEM(shear_offsets.shape, jnp.int32),
            pltpu.VMEM(measured.shape, f32),
            pltpu.VMEM((HALVES, owned * group, width), f32),
            pltpu.VMEM((HALVES, angles * group, width), f32),
            halves(count + cols), halves(cols), halves(cols), halves(count),
            dma((HALVES,)), dma, dma, dma,
        ],
        compiler_params=pltpu.CompilerParams(collective_id=0, has_side_effects=True, vmem_limit_bytes=KERNEL_VMEM),
        name="exchange",
    )(*(pltpu.with_memory_space_constraint(value, pltpu.HBM)
        for value in (volume, ray_weights, shear_weights, shear_offsets, measured)))
    return pl.pallas_call(
        finish,
        out_shape=(jax.ShapeDtypeStruct(measured.shape, f32), jax.ShapeDtypeStruct(volume.shape, f32)),
        in_specs=[vmem] * 3,
        out_specs=(hbm, hbm),
        scratch_shapes=[pltpu.VMEM(volume.shape, f32), pltpu.VMEM(measured.shape, f32), dma, dma],
        compiler_params=pltpu.CompilerParams(vmem_limit_bytes=KERNEL_VMEM),
        name="finish",
    )(columns, pulled, resid)


def solution(mesh):
    placed = (P(None, "row", "col"), P(None, "row"), P(), P(), P("row", None, "col"))
    return jax.shard_map(
        on_device,
        mesh=mesh,
        in_specs=placed,
        out_specs=(P("row", None, "col"), P(None, "row", "col")),
        check_vma=False,
    )
```
